32 devices in a mesh: rep: 4 (over y, x), feat: 8 (over z, core).
Axes of the slice: x: 2, y: 2, z: 4, core: 2. Of those that a mesh axis runs over, the one named last changes fastest.
Arguments:
- basis: float32 [4, 64, 32768], P('rep', None, 'feat'), may hold values from -6 to 6
- stream: bfloat16 [4, 2, 128, 32768], P('rep', None, None, 'feat'), may hold values from -6 to 6
Outputs:
- new_basis: float32 [4, 64, 32768], P('rep', None, 'feat')
The draws below stay inside these ranges and needn't reach their ends.
All inputs are finite; a program needn't handle non-finite values.
Results may differ from the reference program's by a relative error of at most 0.0003.
Values sent between devices are 32-bit elements; how exact they have to be, the bound alone decides.
A program may use at most 64 MiB of HBM per device.

```python
import jax
import jax.numpy as jnp
from jax import lax

RANK = 64
BATCH = 128
STEPS = 2
NF = 32768
REPS = 4


def draw_basis(key, part):
    shape = (REPS, RANK, NF)
    inner = jax.random.fold_in(key, 11)
    values = jax.random.normal(inner, shape, jnp.float32)
    return jnp.clip(values, -6.0, 6.0)


def draw_stream(key, part):
    shape = (REPS, STEPS, BATCH, NF)
    inner = jax.random.fold_in(key, 21)
    values = jax.random.normal(inner, shape, jnp.float32)
    return jnp.clip(values, -6.0, 6.0).astype(jnp.bfloat16)


def setup_inputs(seed: int = 0) -> dict:
    arg_keys = jax.random.split(jax.random.key(seed), 3)
    return {
        "basis": draw_basis(jax.random.fold_in(arg_keys[2], 71), 0),
        "stream": draw_stream(jax.random.fold_in(arg_keys[2], 71), 0),
    }


learn_rate = 0.5

def one_replica(pair):
    start, batches, average = pair
    scale = jnp.sqrt(jnp.float32(NF))
    step_size = learn_rate / BATCH
    current = start
    for step in range(STEPS):
        rows = batches[step].astype(jnp.float32)
        proj = jnp.dot(rows.astype(jnp.float32), current.T.astype(jnp.float32), precision=lax.Precision.HIGHEST, preferred_element_type=jnp.float32) / scale
        cov = jnp.dot(proj.T.astype(jnp.float32), proj.astype(jnp.float32), precision=lax.Precision.HIGHEST, preferred_element_type=jnp.float32)
        drive = jnp.dot(proj.T.astype(jnp.float32), rows.astype(jnp.float32), precision=lax.Precision.HIGHEST, preferred_element_type=jnp.float32)
        shrink = jnp.dot(cov.astype(jnp.float32), current.astype(jnp.float32), precision=lax.Precision.HIGHEST, preferred_element_type=jnp.float32)
        current = current + step_size * (drive - shrink)
    mixed = current + average - start
    gram = jnp.dot(mixed.astype(jnp.float32), mixed.T.astype(jnp.float32), precision=lax.Precision.HIGHEST, preferred_element_type=jnp.float32) / NF
    lower = jnp.linalg.cholesky(gram)
    return lax.linalg.triangular_solve(lower, mixed, left_side=True, lower=True)

def reference(basis, stream):
    average = lax.optimization_barrier(jnp.sum(basis, axis=0)) / REPS

    def apply_one(pair):
        return one_replica((pair[0], pair[1], average))
    return lax.map(apply_one, (basis, stream))
```

```python
import functools

import jax
import jax.numpy as jnp
from jax import lax
from jax.experimental import pallas as pl
from jax.experimental.pallas import tpu as pltpu
from jax.sharding import PartitionSpec as P

learn_rate = 0.5
LANE = 128
PLAN = (2, 18, 3, 1)
SUB = 8
NB = 2
PIECES = 4
LATE = 2
MESH = pl.DeviceIdType.MESH
NN = (((1,), (0,)), ((), ()))
NT = (((1,), (1,)), ((), ()))


def exact_dot(left, right, dims):
    return lax.dot_general(
        left, right, dims, precision=lax.Precision.HIGHEST, preferred_element_type=jnp.float32
    )


def fast_dot(left, right, dims):
    return lax.dot_general(left, right, dims, preferred_element_type=jnp.float32)


def halves(value):
    high = value.astype(jnp.bfloat16)
    low = (value - high.astype(jnp.float32)).astype(jnp.bfloat16)
    return high, low


def gather_kernel(
    reps, feats, rank, rows, cols, total_feat,
    basis_hbm, stream_hbm, gram_ref, mh_ref, ml_ref,
    m_ref, w_ref, x_ref, whl_ref, sums_refs, recv_refs, av_ref,
    pay_ref, half_recv, half_sum, z_recv, full_ref,
    g_ref, g_core, g_recv,
    load_sem, ring_send, ring_recv, core_send, core_recv, z_send, z_recv_sem,
    gz_send, gz_recv, gx_send, gx_recv, hello_sem,
):
    bits = reps.bit_length() - 1
    chunk = LANE * reps
    chunks = cols // chunk
    zs = feats // 2
    me = lax.axis_index("rep")
    feat = lax.axis_index("feat")
    core = feat % 2
    zpos = feat // 2
    eta = learn_rate / rows
    scale = jnp.sqrt(jnp.float32(total_feat))

    loads = []
    for c in range(chunks):
        cut = slice(c * chunk, (c + 1) * chunk)
        loads.append(pltpu.make_async_copy(basis_hbm.at[:, cut], w_ref.at[:, cut], load_sem.at[c]))
        loads[c].start()
    load_x = pltpu.make_async_copy(stream_hbm, x_ref, load_sem.at[chunks])
    load_x.start()

    def rep_peer(b):
        bit = (me // (1 << b)) % 2
        return me + (1 - 2 * bit) * (1 << b), bit

    rep_ids = [(rep_peer(b)[0], feat) for b in range(bits)]
    core_id = (me, feat + 1 - 2 * core)
    z_ids = [(me, ((zpos + d) % zs) * 2 + core) for d in range(1, zs)]

    beside = (zpos > 0).astype(jnp.int32) + (zpos < zs - 1).astype(jnp.int32)

    def tell_beside(sem):
        for ahead, there in ((-1, zpos > 0), (1, zpos < zs - 1)):

            @pl.when(there)
            def _():
                pl.semaphore_signal(
                    sem, inc=1, device_id=(me, feat + 2 * ahead), device_id_type=MESH
                )

    barrier = pltpu.get_barrier_semaphore()
    for peer in rep_ids + [core_id]:
        pl.semaphore_signal(barrier, inc=1, device_id=peer, device_id_type=MESH)
    tell_beside(barrier)
    pl.semaphore_wait(barrier, bits + 1 + beside)

    def remote(src, dst, send_sem, recv_sem, peer):
        copy = pltpu.make_async_remote_copy(
            src_ref=src, dst_ref=dst, send_sem=send_sem, recv_sem=recv_sem,
            device_id=peer, device_id_type=MESH,
        )
        copy.start()
        return copy

    started = []

    def at(off, width):
        return pl.ds(pl.multiple_of(off, LANE), width)

    def order(c):
        return [(c + i) % bits for i in range(bits)]

    keeps = []
    for c in range(chunks):
        off = c * chunk
        rec = []
        for i, b in enumerate(order(c)):
            width = chunk >> (i + 1)
            bit = rep_peer(b)[1]
            off = off + bit * width
            rec.append(off)
        keeps.append(rec)

    ring = {}

    def send_scatter(c, i):
        b = order(c)[i]
        width = chunk >> (i + 1)
        bit = rep_peer(b)[1]
        other = (1 - bit) * width
        if i == 0:
            src = w_ref.at[:, at(c * chunk + other, width)]
        else:
            src = sums_refs[i - 1].at[:, at(c * 2 * width + other, width)]
        dst = recv_refs[i].at[:, c * width:(c + 1) * width]
        ring[c, i] = remote(src, dst, ring_send.at[i, c], ring_recv.at[i, c], rep_ids[b])

    def take_scatter(c, i):
        b = order(c)[i]
        width = chunk >> (i + 1)
        bit = rep_peer(b)[1]
        ring[c, i].wait_recv()
        if i == 0:
            own = w_ref[:, at(c * chunk + bit * width, width)]
        else:
            own = sums_refs[i - 1][:, at(c * 2 * width + bit * width, width)]
        total = own + recv_refs[i][:, c * width:(c + 1) * width]
        if i == bits - 1:
            av_ref[:, at(keeps[c][i], width)] = total / reps
        else:
            sums_refs[i][:, c * width:(c + 1) * width] = total

    def send_gather(c, i):
        s = bits - 1 - i
        b = order(c)[s]
        width = chunk >> (s + 1)
        piece = av_ref.at[:, at(keeps[c][s], width)]
        k = bits + i
        ring[c, k] = remote(piece, piece, ring_send.at[k, c], ring_recv.at[k, c], rep_ids[b])

    for c in range(chunks):
        loads[c].wait()
        send_scatter(c, 0)
    rounds = zs - 2
    if rounds > 0:
        tell_beside(hello_sem.at[0])

    def step(c, i):
        if i < bits:
            take_scatter(c, i)
        else:
            ring[c, i].wait_recv()
        if i + 1 < bits:
            send_scatter(c, i + 1)
        elif i + 1 < 2 * bits:
            send_gather(c, i + 1 - bits)

    pending = [(c, i) for i in range(2 * bits - 1) for c in range(chunks)]
    place = [0]

    def advance(count):
        for _ in range(count):
            if place[0] < len(pending):
                step(*pending[place[0]])
                place[0] += 1

    high, low = halves(w_ref[...])
    whl_ref[0:rank, :] = high
    whl_ref[rank:2 * rank, :] = low
    load_x.wait()
    x_all = x_ref[...]
    wx = fast_dot(whl_ref[...], x_all, NT)
    wx = wx[0:rank] + wx[rank:2 * rank]
    pay_ref[0:rank, :] = wx[:, 0:rows]
    pay_ref[rank:2 * rank, :] = wx[:, rows:2 * rows]
    pay_ref[2 * rank:2 * rank + rows, :] = fast_dot(x_ref[0:rows, :], x_ref[rows:2 * rows, :], NT)

    half = rank + rows // 2
    give = pl.ds(pl.multiple_of((1 - core) * half, 8), half)
    keep = pl.ds(pl.multiple_of(core * half, 8), half)
    core_copy = remote(pay_ref.at[give, :], half_recv, core_send.at[0], core_recv.at[0], core_id)
    advance(PLAN[0])
    core_copy.wait_recv()
    half_sum[...] = pay_ref[keep, :] + half_recv[...]
    for k in range(rounds):
        pl.semaphore_wait(hello_sem.at[k], beside)
        if k + 1 < rounds:
            tell_beside(hello_sem.at[k + 1])
    z_copies = [
        remote(half_sum, z_recv.at[d], z_send.at[d], z_recv_sem.at[d], z_ids[d])
        for d in range(zs - 1)
    ]
    started.append(core_copy)
    started.extend(z_copies)
    advance(PLAN[1])
    total = half_sum[...]
    for d in range(zs - 1):
        z_copies[d].wait_recv()
        total = total + z_recv[d]
    full_ref[keep, :] = total
    share = remote(full_ref.at[keep, :], full_ref.at[keep, :], core_send.at[1], core_recv.at[1], core_id)
    started.append(share)
    advance(PLAN[2])
    share.wait_recv()

    first = full_ref[0:rank, :]
    second = full_ref[rank:2 * rank, :]
    cross = full_ref[2 * rank:2 * rank + rows, :]
    proj0 = first / scale
    cov0 = exact_dot(proj0, proj0, NT)
    drive1 = exact_dot(proj0, cross, NN)
    proj1 = (second + eta * (drive1 - exact_dot(cov0, second, NN))) / scale
    cov1 = exact_dot(proj1, proj1, NT)
    advance(PLAN[3])
    k_w = eta * (eta * exact_dot(cov1, cov0, NN) - cov0 - cov1)
    k_x0 = eta * (proj0 - eta * exact_dot(cov1, proj0, NN))
    k_x1 = eta * proj1
    kwh, kwl = halves(k_w)
    kx = jnp.concatenate([k_x0, k_x1], axis=1)
    kxh, kxl = halves(kx)
    kx2 = jnp.concatenate([kxh, kxl], axis=0)
    kw2 = jnp.concatenate([kwh, kwl], axis=0)

    def unmixed(c):
        cut = slice(c * chunk, (c + 1) * chunk)
        part = fast_dot(kx2, x_ref[:, cut], NN) + fast_dot(kw2, whl_ref[0:rank, cut], NN)
        part = part[0:rank] + part[rank:2 * rank] + fast_dot(kwh, whl_ref[rank:2 * rank, cut], NN)
        m_ref[:, cut] = part

    for c in range(chunks):
        unmixed(c)
        advance(1)
    advance(len(pending))

    slim = [jnp.zeros((2 * rank, rank), jnp.float32)]
    full = [jnp.zeros((rank, 2 * rank), jnp.float32)]

    def mix(off, width, late):
        cut = at(off, width)
        mh, ml = halves(m_ref[:, cut] + av_ref[:, cut])
        mh_ref[:, cut] = mh
        ml_ref[:, cut] = ml
        both = jnp.concatenate([mh, ml], axis=0)
        if late:
            part = fast_dot(both, jnp.concatenate([mh, mh], axis=0), NT)
            part = part[0:rank] + part[rank:2 * rank]
            full[0] = full[0] + (part + fast_dot(mh, jnp.concatenate([ml, ml], axis=0), NT))
        else:
            slim[0] = slim[0] + fast_dot(both, mh, NT)

    wide = chunk // 2
    for c in range(chunks):
        mix(keeps[c][0], wide, False)
    for c in range(chunks):
        if c == chunks - LATE:
            low_part = slim[0][rank:2 * rank]
            early = slim[0][0:rank] + (low_part + low_part.T)
            full[0] = full[0] + jnp.concatenate([early, early], axis=1)
        ring[c, 2 * bits - 1].wait_recv()
        mix(2 * c * chunk + wide - keeps[c][0], wide, c >= chunks - LATE)
    hr = rank // 2
    gram = full[0] / total_feat
    lane = lax.broadcasted_iota(jnp.int32, (hr, 2 * rank), 1)
    g_ref[...] = jnp.where(lane < rank, gram[0:hr], gram[hr:rank])
    upper = (2 * zpos) // zs
    g_copies = []
    for j in range(zs - 1):
        far = upper * (j + (j >= zpos).astype(jnp.int32))
        near = (1 - upper) * (zs - 1 - j - (zs - 1 - j <= zpos).astype(jnp.int32))
        peer = far + near
        slot = (peer - zpos + zs) % zs - 1
        for k in range(2):
            other = (core + k) % 2
            g_copies.append(remote(
                g_ref, g_recv.at[k, slot], gz_send.at[k, slot], gz_recv.at[k, slot],
                (me, peer * 2 + other),
            ))
    gc = remote(g_ref, g_core, gx_send.at[0], gx_recv.at[0], core_id)
    gc.wait_recv()
    total = g_ref[...] + g_core[...]
    for copy in g_copies:
        copy.wait_recv()
    for k in range(2):
        for d in range(zs - 1):
            total = total + g_recv[k, d]
    gram_ref[...] = total
    for copy in started + [gc] + g_copies + list(ring.values()):
        copy.wait_send()


def lanes(block, lane):
    return jnp.broadcast_to(block[:, lane:lane + 1], block.shape)

def row(block, r):
    return jnp.broadcast_to(block[r:r + 1, :], block.shape)

def panel(blocks, first, nb, col, ids):
    w = SUB * nb
    last = len(blocks)
    own = [blocks[first + v] for v in range(nb)]
    d = [[lanes(own[v], col + k) for v in range(nb)] for k in range(w)]
    c = {i: [lanes(blocks[i], col + k) for k in range(w)] for i in range(first + nb, last)}
    done = []
    for p in range(0, w, 2):
        v, s = divmod(p, SUB)
        a00, a10, a11 = row(d[p][v], s), row(d[p][v], s + 1), row(d[p + 1][v], s + 1)
        idet = 1.0 / (a00 * a11 - a10 * a10)
        i00, i01, i11 = a11 * idet, -(a10 * idet), a00 * idet
        at0, at1 = ids == s, ids == s + 1

        def step(x):
            t0, t1 = row(x[v], s), row(x[v], s + 1)
            z0 = i00 * t0 + i01 * t1
            z1 = i01 * t0 + i11 * t1
            out = []
            for u in range(nb):
                new = x[u] - (d[p][u] * z0 + d[p + 1][u] * z1)
                if u == v:
                    new = jnp.where(at0, z0, jnp.where(at1, z1, new))
                out.append(new)
            return t0, t1, out

        r0, r1, new_own = step(own)
        ratio = a10 / a00
        done.append(r0 * lax.rsqrt(a00))
        done.append((r1 - ratio * r0) * lax.rsqrt(a11 - ratio * a10))
        new_d = {k: step(d[k])[2] for k in range(p + 2, w)}
        own = new_own
        for k in new_d:
            d[k] = new_d[k]
    if c:
        z = [row(own[p // SUB], p % SUB) for p in range(w)]
        for i in c:
            parts = [c[i][p] * z[p] for p in range(w)]
            while len(parts) > 1:
                parts = [parts[q] + parts[q + 1] for q in range(0, len(parts), 2)]
            blocks[i] = blocks[i] - parts[0]
    res = []
    for v in range(nb):
        out = done[v * SUB]
        for s in range(1, SUB):
            out = jnp.where(ids == s, done[v * SUB + s], out)
        res.append(out)
    return res

def solve_kernel(rank, cols, gram_ref, mh_ref, ml_ref, out_hbm, ph_ref, pl_ref, o_ref, out_sem):
    hr = rank // 2
    n = rank // SUB
    half = n // 2
    lane = lax.broadcasted_iota(jnp.int32, (SUB, 2 * rank), 1)
    ids = lax.broadcasted_iota(jnp.int32, (SUB, 2 * rank), 0)
    both = gram_ref[...]
    zero = jnp.zeros((SUB, rank), jnp.float32)
    top = [both[i * SUB:(i + 1) * SUB, :] for i in range(half)]
    low = [jnp.concatenate([t[:, rank:2 * rank], zero], axis=1) for t in top]
    blocks = [
        jnp.where(lane < rank, top[i], jnp.where(lane == rank + ids + i * SUB, 1.0, 0.0))
        for i in range(half)
    ] + low
    width = cols // PIECES
    outs = []

    def send(lo, p):
        cut = slice(p * width, (p + 1) * width)
        copy = pltpu.make_async_copy(
            o_ref.at[lo:lo + hr, cut], out_hbm.at[lo:lo + hr, cut], out_sem.at[len(outs)]
        )
        copy.start()
        outs.append(copy)

    def eliminate(first):
        scaled = []
        for b in range(first, first + half, NB):
            scaled += panel(blocks, b, NB, b * SUB, ids)
        return scaled

    scaled = eliminate(0)
    left = jnp.concatenate(scaled + blocks[half:], axis=0)[:, rank:rank + hr]
    th, tl = halves(left)
    thl = jnp.concatenate([th, tl], axis=0)
    for p in range(PIECES):
        cut = slice(p * width, (p + 1) * width)
        part = fast_dot(thl, mh_ref[0:hr, cut], NN)
        part = part[0:rank] + part[rank:2 * rank] + fast_dot(th, ml_ref[0:hr, cut], NN)
        o_ref[0:hr, cut] = part[0:hr]
        send(0, p)
        rest = part[hr:rank] + mh_ref[hr:rank, cut].astype(jnp.float32)
        rest = rest + ml_ref[hr:rank, cut].astype(jnp.float32)
        ph_ref[:, cut], pl_ref[:, cut] = halves(rest)
    for i in range(half):
        unit = jnp.where(lane == ids + i * SUB, 1.0, 0.0)
        blocks[half + i] = jnp.where(lane < hr, unit, blocks[half + i])
    left = jnp.concatenate(eliminate(half), axis=0)[:, 0:hr]
    th, tl = halves(left)
    thl = jnp.concatenate([th, tl], axis=0)
    for p in range(PIECES):
        cut = slice(p * width, (p + 1) * width)
        part = fast_dot(thl, ph_ref[:, cut], NN)
        o_ref[hr:rank, cut] = part[0:hr] + part[hr:rank] + fast_dot(th, pl_ref[:, cut], NN)
        send(hr, p)
    for copy in outs:
        copy.wait()


def per_device(basis, stream):
    reps = lax.axis_size("rep")
    feats = lax.axis_size("feat")
    start = basis[0]
    steps, rows, cols = stream.shape[1:]
    batches = stream[0].reshape(steps * rows, cols)
    rank = start.shape[0]
    bits = reps.bit_length() - 1
    chunk = LANE * reps
    chunks = cols // chunk
    zs = feats // 2
    half = rank + rows // 2
    f32 = jnp.float32
    vm = pltpu.VMEM
    hr = rank // 2
    dma = pltpu.SemaphoreType.DMA
    gram, mh, ml = pl.pallas_call(
        functools.partial(gather_kernel, reps, feats, rank, rows, cols, cols * feats),
        out_shape=(
            pltpu.VMEM((hr, 2 * rank), f32),
            pltpu.VMEM((rank, cols), jnp.bfloat16),
            pltpu.VMEM((rank, cols), jnp.bfloat16),
        ),
        in_specs=[pl.BlockSpec(memory_space=pl.ANY)] * 2,
        out_specs=(pl.BlockSpec(memory_space=pltpu.VMEM),) * 3,
        scratch_shapes=[
            vm((rank, cols), f32),
            vm((rank, cols), f32),
            vm((steps * rows, cols), jnp.bfloat16),
            vm((2 * rank, cols), jnp.bfloat16),
            [vm((rank, cols >> (i + 1)), f32) for i in range(bits)],
            [vm((rank, cols >> (i + 1)), f32) for i in range(bits)],
            vm((rank, cols), f32),
            vm((2 * half, rows), f32),
            vm((half, rows), f32),
            vm((half, rows), f32),
            vm((zs - 1, half, rows), f32),
            vm((2 * half, rows), f32),
            vm((hr, 2 * rank), f32),
            vm((hr, 2 * rank), f32),
            vm((2, zs - 1, hr, 2 * rank), f32),
            dma((chunks + 1,)),
            dma((2 * bits, chunks)),
            dma((2 * bits, chunks)),
            dma((2,)),
            dma((2,)),
            dma((zs - 1,)),
            dma((zs - 1,)),
            dma((2, zs - 1)),
            dma((2, zs - 1)),
            dma((1,)),
            dma((1,)),
            pltpu.SemaphoreType.REGULAR((max(zs - 2, 1),)),
        ],
        compiler_params=pltpu.CompilerParams(collective_id=0, has_side_effects=True),
    )(start, batches)
    result = pl.pallas_call(
        functools.partial(solve_kernel, rank, cols),
        out_shape=jax.ShapeDtypeStruct((rank, cols), f32),
        in_specs=[pl.BlockSpec(memory_space=pltpu.VMEM)] * 3,
        out_specs=pl.BlockSpec(memory_space=pl.ANY),
        scratch_shapes=[
            vm((hr, cols), jnp.bfloat16),
            vm((hr, cols), jnp.bfloat16),
            vm((rank, cols), f32),
            dma((2 * PIECES,)),
        ],
    )(
        pltpu.with_memory_space_constraint(gram, pltpu.VMEM),
        pltpu.with_memory_space_constraint(mh, pltpu.VMEM),
        pltpu.with_memory_space_constraint(ml, pltpu.VMEM),
    )
    return result[None]


def solution(mesh):
    placed = (P("rep", None, "feat"), P("rep", None, None, "feat"))
    return jax.shard_map(
        per_device, mesh=mesh, in_specs=placed, out_specs=P("rep", None, "feat"), check_vma=False
    )
```

```python
import functools

import jax
import jax.numpy as jnp
from jax import lax
from jax.experimental import pallas as pl
from jax.experimental.pallas import tpu as pltpu
from jax.sharding import PartitionSpec as P

learn_rate = 0.5
LANE = 128
PLAN = (2, 18, 3, 1)
SUB = 8
NB = 2
PIECES = 4
LATE = 2
MESH = pl.DeviceIdType.MESH
NN = (((1,), (0,)), ((), ()))
NT = (((1,), (1,)), ((), ()))


def exact_dot(left, right, dims):
    return lax.dot_general(
        left, right, dims, precision=lax.Precision.HIGHEST, preferred_element_type=jnp.float32
    )


def fast_dot(left, right, dims):
    return lax.dot_general(left, right, dims, preferred_element_type=jnp.float32)


def halves(value):
    high = value.astype(jnp.bfloat16)
    low = (value - high.astype(jnp.float32)).astype(jnp.bfloat16)
    return high, low


def gather_kernel(
    reps, feats, rank, rows, cols, total_feat,
    basis_hbm, stream_hbm, gram_ref, mh_ref, ml_ref,
    m_ref, w_ref, x_ref, whl_ref, sums_refs, recv_refs, av_ref,
    pay_ref, half_recv, half_sum, z_recv, full_ref,
    g_ref, g_core, g_recv,
    load_sem, ring_send, ring_recv, core_send, core_recv, z_send, z_recv_sem,
    gz_send, gz_recv, gx_send, gx_recv, hello_sem,
):
    bits = reps.bit_length() - 1
    chunk = LANE * reps
    chunks = cols // chunk
    zs = feats // 2
    me = lax.axis_index("rep")
    feat = lax.axis_index("feat")
    core = feat % 2
    zpos = feat // 2
    eta = learn_rate / rows
    scale = jnp.sqrt(jnp.float32(total_feat))

    loads = []
    for c in range(chunks):
        cut = slice(c * chunk, (c + 1) * chunk)
        loads.append(pltpu.make_async_copy(basis_hbm.at[:, cut], w_ref.at[:, cut], load_sem.at[c]))
        loads[c].start()
    load_x = pltpu.make_async_copy(stream_hbm, x_ref, load_sem.at[chunks])
    load_x.start()

    def rep_peer(b):
        bit = (me // (1 << b)) % 2
        return me + (1 - 2 * bit) * (1 << b), bit

    rep_ids = [(rep_peer(b)[0], feat) for b in range(bits)]
    core_id = (me, feat + 1 - 2 * core)
    z_ids = [(me, ((zpos + d) % zs) * 2 + core) for d in range(1, zs)]

    beside = (zpos > 0).astype(jnp.int32) + (zpos < zs - 1).astype(jnp.int32)

    def tell_beside(sem):
        for ahead, there in ((-1, zpos > 0), (1, zpos < zs - 1)):

            @pl.when(there)
            def _():
                pl.semaphore_signal(
                    sem, inc=1, device_id=(me, feat + 2 * ahead), device_id_type=MESH
                )

    barrier = pltpu.get_barrier_semaphore()
    for peer in rep_ids + [core_id]:
        pl.semaphore_signal(barrier, inc=1, device_id=peer, device_id_type=MESH)
    tell_beside(barrier)
    pl.semaphore_wait(barrier, bits + 1 + beside)

    def remote(src, dst, send_sem, recv_sem, peer):
        copy = pltpu.make_async_remote_copy(
            src_ref=src, dst_ref=dst, send_sem=send_sem, recv_sem=recv_sem,
            device_id=peer, device_id_type=MESH,
        )
        copy.start()
        return copy

    started = []

    def at(off, width):
        return pl.ds(pl.multiple_of(off, LANE), width)

    def order(c):
        return [(c + i) % bits for i in range(bits)]

    keeps = []
    for c in range(chunks):
        off = c * chunk
        rec = []
        for i, b in enumerate(order(c)):
            width = chunk >> (i + 1)
            bit = rep_peer(b)[1]
            off = off + bit * width
            rec.append(off)
        keeps.append(rec)

    ring = {}

    def send_scatter(c, i):
        b = order(c)[i]
        width = chunk >> (i + 1)
        bit = rep_peer(b)[1]
        other = (1 - bit) * width
        if i == 0:
            src = w_ref.at[:, at(c * chunk + other, width)]
        else:
            src = sums_refs[i - 1].at[:, at(c * 2 * width + other, width)]
        dst = recv_refs[i].at[:, c * width:(c + 1) * width]
        ring[c, i] = remote(src, dst, ring_send.at[i, c], ring_recv.at[i, c], rep_ids[b])

    def take_scatter(c, i):
        b = order(c)[i]
        width = chunk >> (i + 1)
        bit = rep_peer(b)[1]
        ring[c, i].wait_recv()
        if i == 0:
            own = w_ref[:, at(c * chunk + bit * width, width)]
        else:
            own = sums_refs[i - 1][:, at(c * 2 * width + bit * width, width)]
        total = own + recv_refs[i][:, c * width:(c + 1) * width]
        if i == bits - 1:
            av_ref[:, at(keeps[c][i], width)] = total / reps
        else:
            sums_refs[i][:, c * width:(c + 1) * width] = total

    def send_gather(c, i):
        s = bits - 1 - i
        b = order(c)[s]
        width = chunk >> (s + 1)
        piece = av_ref.at[:, at(keeps[c][s], width)]
        k = bits + i
        ring[c, k] = remote(piece, piece, ring_send.at[k, c], ring_recv.at[k, c], rep_ids[b])

    for c in range(chunks):
        loads[c].wait()
        send_scatter(c, 0)
    rounds = zs - 2
    if rounds > 0:
        tell_beside(hello_sem.at[0])

    def step(c, i):
        if i < bits:
            take_scatter(c, i)
        else:
            ring[c, i].wait_recv()
        if i + 1 < bits:
            send_scatter(c, i + 1)
        elif i + 1 < 2 * bits:
            send_gather(c, i + 1 - bits)

    pending = [(c, i) for i in range(2 * bits - 1) for c in range(chunks)]
    place = [0]

    def advance(count):
        for _ in range(count):
            if place[0] < len(pending):
                step(*pending[place[0]])
                place[0] += 1

    high, low = halves(w_ref[...])
    whl_ref[0:rank, :] = high
    whl_ref[rank:2 * rank, :] = low
    load_x.wait()
    x_all = x_ref[...]
    wx = fast_dot(whl_ref[...], x_all, NT)
    wx = wx[0:rank] + wx[rank:2 * rank]
    pay_ref[0:rank, :] = wx[:, 0:rows]
    pay_ref[rank:2 * rank, :] = wx[:, rows:2 * rows]
    pay_ref[2 * rank:2 * rank + rows, :] = fast_dot(x_ref[0:rows, :], x_ref[rows:2 * rows, :], NT)

    half = rank + rows // 2
    give = pl.ds(pl.multiple_of((1 - core) * half, 8), half)
    keep = pl.ds(pl.multiple_of(core * half, 8), half)
    core_copy = remote(pay_ref.at[give, :], half_recv, core_send.at[0], core_recv.at[0], core_id)
    advance(PLAN[0])
    core_copy.wait_recv()
    half_sum[...] = pay_ref[keep, :] + half_recv[...]
    for k in range(rounds):
        pl.semaphore_wait(hello_sem.at[k], beside)
        if k + 1 < rounds:
            tell_beside(hello_sem.at[k + 1])
    z_copies = [
        remote(half_sum, z_recv.at[d], z_send.at[d], z_recv_sem.at[d], z_ids[d])
        for d in range(zs - 1)
    ]
    started.append(core_copy)
    started.extend(z_copies)
    advance(PLAN[1])
    total = half_sum[...]
    for d in range(zs - 1):
        z_copies[d].wait_recv()
        total = total + z_recv[d]
    full_ref[keep, :] = total
    share = remote(full_ref.at[keep, :], full_ref.at[keep, :], core_send.at[1], core_recv.at[1], core_id)
    started.append(share)
    advance(PLAN[2])
    share.wait_recv()

    first = full_ref[0:rank, :]
    second = full_ref[rank:2 * rank, :]
    cross = full_ref[2 * rank:2 * rank + rows, :]
    proj0 = first / scale
    cov0 = exact_dot(proj0, proj0, NT)
    drive1 = exact_dot(proj0, cross, NN)
    proj1 = (second + eta * (drive1 - exact_dot(cov0, second, NN))) / scale
    cov1 = exact_dot(proj1, proj1, NT)
    advance(PLAN[3])
    k_w = eta * (eta * exact_dot(cov1, cov0, NN) - cov0 - cov1)
    k_x0 = eta * (proj0 - eta * exact_dot(cov1, proj0, NN))
    k_x1 = eta * proj1
    kwh, kwl = halves(k_w)
    kx = jnp.concatenate([k_x0, k_x1], axis=1)
    kxh, kxl = halves(kx)
    kx2 = jnp.concatenate([kxh, kxl], axis=0)
    kw2 = jnp.concatenate([kwh, kwl], axis=0)

    def unmixed(c):
        cut = slice(c * chunk, (c + 1) * chunk)
        part = fast_dot(kx2, x_ref[:, cut], NN) + fast_dot(kw2, whl_ref[0:rank, cut], NN)
        part = part[0:rank] + part[rank:2 * rank] + fast_dot(kwh, whl_ref[rank:2 * rank, cut], NN)
        m_ref[:, cut] = part

    for c in range(chunks):
        unmixed(c)
        advance(1)
    advance(len(pending))

    slim = [jnp.zeros((2 * rank, rank), jnp.float32)]
    full = [jnp.zeros((rank, 2 * rank), jnp.float32)]

    def mix(off, width, late):
        cut = at(off, width)
        mh, ml = halves(m_ref[:, cut] + av_ref[:, cut])
        mh_ref[:, cut] = mh
        ml_ref[:, cut] = ml
        both = jnp.concatenate([mh, ml], axis=0)
        if late:
            part = fast_dot(both, jnp.concatenate([mh, mh], axis=0), NT)
            part = part[0:rank] + part[rank:2 * rank]
            full[0] = full[0] + (part + fast_dot(mh, jnp.concatenate([ml, ml], axis=0), NT))
        else:
            slim[0] = slim[0] + fast_dot(both, mh, NT)

    wide = chunk // 2
    for c in range(chunks):
        mix(keeps[c][0], wide, False)
    for c in range(chunks):
        if c == chunks - LATE:
            low_part = slim[0][rank:2 * rank]
            early = slim[0][0:rank] + (low_part + low_part.T)
            full[0] = full[0] + jnp.concatenate([early, early], axis=1)
        ring[c, 2 * bits - 1].wait_recv()
        mix(2 * c * chunk + wide - keeps[c][0], wide, c >= chunks - LATE)
    hr = rank // 2
    gram = full[0] / total_feat
    lane = lax.broadcasted_iota(jnp.int32, (hr, 2 * rank), 1)
    g_ref[...] = jnp.where(lane < rank, gram[0:hr], gram[hr:rank])
    upper = (2 * zpos) // zs
    g_copies = []
    for j in range(zs - 1):
        far = upper * (j + (j >= zpos).astype(jnp.int32))
        near = (1 - upper) * (zs - 1 - j - (zs - 1 - j <= zpos).astype(jnp.int32))
        peer = far + near
        slot = (peer - zpos + zs) % zs - 1
        for k in range(2):
            other = (core + k) % 2
            g_copies.append(remote(
                g_ref, g_recv.at[k, slot], gz_send.at[k, slot], gz_recv.at[k, slot],
                (me, peer * 2 + other),
            ))
    gc = remote(g_ref, g_core, gx_send.at[0], gx_recv.at[0], core_id)
    gc.wait_recv()
    total = g_ref[...] + g_core[...]
    for copy in g_copies:
        copy.wait_recv()
    for k in range(2):
        for d in range(zs - 1):
            total = total + g_recv[k, d]
    gram_ref[...] = total
    for copy in started + [gc] + g_copies + list(ring.values()):
        copy.wait_send()


def lanes(block, lane):
    return jnp.broadcast_to(block[:, lane:lane + 1], block.shape)

def row(block, r):
    return jnp.broadcast_to(block[r:r + 1, :], block.shape)

def panel(blocks, first, nb, col, ids):
    w = SUB * nb
    last = len(blocks)
    own = [blocks[first + v] for v in range(nb)]
    keep = ids < w
    d = [[jnp.where(keep, lanes(own[v], col + k), 0.0) for v in range(nb)] for k in range(w)]
    c = {i: [lanes(blocks[i], col + k) for k in range(w)] for i in range(first + nb, last)}
    done = []
    for p in range(0, w, 2):
        v, s = divmod(p, SUB)
        a00, a10, a11 = row(d[p][v], s), row(d[p][v], s + 1), row(d[p + 1][v], s + 1)
        idet = 1.0 / (a00 * a11 - a10 * a10)
        i00, i01, i11 = a11 * idet, -(a10 * idet), a00 * idet
        at0, pair = ids == s, (ids == s) | (ids == s + 1)
        e0 = [d[p][u] * i00 + d[p + 1][u] * i01 for u in range(nb)]
        e1 = [d[p][u] * i01 + d[p + 1][u] * i11 for u in range(nb)]
        e0[v] = jnp.where(pair, jnp.where(at0, -i00, -i01), e0[v])
        e1[v] = jnp.where(pair, jnp.where(at0, -i01, -i11), e1[v])

        def step(x):
            t0, t1 = row(x[v], s), row(x[v], s + 1)
            base = [jnp.where(pair, 0.0, x[u]) if u == v else x[u] for u in range(nb)]
            return t0, t1, [base[u] - (e0[u] * t0 + e1[u] * t1) for u in range(nb)]

        r0, r1, own = step(own)
        ratio = a10 / a00
        done.append(r0 * lax.rsqrt(a00))
        done.append((r1 - ratio * r0) * lax.rsqrt(a11 - ratio * a10))
        for k in range(p + 2, w):
            d[k] = step(d[k])[2]
    if c:
        z = [row(own[p // SUB], p % SUB) for p in range(w)]
        for i in c:
            parts = [c[i][p] * z[p] for p in range(w)]
            while len(parts) > 1:
                parts = [parts[q] + parts[q + 1] for q in range(0, len(parts), 2)]
            blocks[i] = blocks[i] - parts[0]
    res = []
    for v in range(nb):
        out = done[v * SUB]
        for s in range(1, SUB):
            out = jnp.where(ids == s, done[v * SUB + s], out)
        res.append(out)
    return res
def solve_kernel(rank, cols, gram_ref, mh_ref, ml_ref, out_hbm, ph_ref, pl_ref, o_ref, out_sem):
    hr = rank // 2
    n = rank // SUB
    half = n // 2
    lane = lax.broadcasted_iota(jnp.int32, (SUB, 2 * rank), 1)
    ids = lax.broadcasted_iota(jnp.int32, (SUB, 2 * rank), 0)
    both = gram_ref[...]
    zero = jnp.zeros((SUB, rank), jnp.float32)
    top = [both[i * SUB:(i + 1) * SUB, :] for i in range(half)]
    low = [jnp.concatenate([t[:, rank:2 * rank], zero], axis=1) for t in top]
    blocks = [
        jnp.where(lane < rank, top[i], jnp.where(lane == rank + ids + i * SUB, 1.0, 0.0))
        for i in range(half)
    ] + low
    width = cols // PIECES
    outs = []

    def send(lo, p):
        cut = slice(p * width, (p + 1) * width)
        copy = pltpu.make_async_copy(
            o_ref.at[lo:lo + hr, cut], out_hbm.at[lo:lo + hr, cut], out_sem.at[len(outs)]
        )
        copy.start()
        outs.append(copy)

    def eliminate(first):
        scaled = []
        for b in range(first, first + half, NB):
            scaled += panel(blocks, b, NB, b * SUB, ids)
        return scaled

    scaled = eliminate(0)
    left = jnp.concatenate(scaled + blocks[half:], axis=0)[:, rank:rank + hr]
    th, tl = halves(left)
    thl = jnp.concatenate([th, tl], axis=0)
    for p in range(PIECES):
        cut = slice(p * width, (p + 1) * width)
        part = fast_dot(thl, mh_ref[0:hr, cut], NN)
        part = part[0:rank] + part[rank:2 * rank] + fast_dot(th, ml_ref[0:hr, cut], NN)
        o_ref[0:hr, cut] = part[0:hr]
        send(0, p)
        rest = part[hr:rank] + mh_ref[hr:rank, cut].astype(jnp.float32)
        rest = rest + ml_ref[hr:rank, cut].astype(jnp.float32)
        ph_ref[:, cut], pl_ref[:, cut] = halves(rest)
    for i in range(half):
        unit = jnp.where(lane == ids + i * SUB, 1.0, 0.0)
        blocks[half + i] = jnp.where(lane < hr, unit, blocks[half + i])
    left = jnp.concatenate(eliminate(half), axis=0)[:, 0:hr]
    th, tl = halves(left)
    thl = jnp.concatenate([th, tl], axis=0)
    for p in range(PIECES):
        cut = slice(p * width, (p + 1) * width)
        part = fast_dot(thl, ph_ref[:, cut], NN)
        o_ref[hr:rank, cut] = part[0:hr] + part[hr:rank] + fast_dot(th, pl_ref[:, cut], NN)
        send(hr, p)
    for copy in outs:
        copy.wait()


def per_device(basis, stream):
    reps = lax.axis_size("rep")
    feats = lax.axis_size("feat")
    start = basis[0]
    steps, rows, cols = stream.shape[1:]
    batches = stream[0].reshape(steps * rows, cols)
    rank = start.shape[0]
    bits = reps.bit_length() - 1
    chunk = LANE * reps
    chunks = cols // chunk
    zs = feats // 2
    half = rank + rows // 2
    f32 = jnp.float32
    vm = pltpu.VMEM
    hr = rank // 2
    dma = pltpu.SemaphoreType.DMA
    gram, mh, ml = pl.pallas_call(
        functools.partial(gather_kernel, reps, feats, rank, rows, cols, cols * feats),
        out_shape=(
            pltpu.VMEM((hr, 2 * rank), f32),
            pltpu.VMEM((rank, cols), jnp.bfloat16),
            pltpu.VMEM((rank, cols), jnp.bfloat16),
        ),
        in_specs=[pl.BlockSpec(memory_space=pl.ANY)] * 2,
        out_specs=(pl.BlockSpec(memory_space=pltpu.VMEM),) * 3,
        scratch_shapes=[
            vm((rank, cols), f32),
            vm((rank, cols), f32),
            vm((steps * rows, cols), jnp.bfloat16),
            vm((2 * rank, cols), jnp.bfloat16),
            [vm((rank, cols >> (i + 1)), f32) for i in range(bits)],
            [vm((rank, cols >> (i + 1)), f32) for i in range(bits)],
            vm((rank, cols), f32),
            vm((2 * half, rows), f32),
            vm((half, rows), f32),
            vm((half, rows), f32),
            vm((zs - 1, half, rows), f32),
            vm((2 * half, rows), f32),
            vm((hr, 2 * rank), f32),
            vm((hr, 2 * rank), f32),
            vm((2, zs - 1, hr, 2 * rank), f32),
            dma((chunks + 1,)),
            dma((2 * bits, chunks)),
            dma((2 * bits, chunks)),
            dma((2,)),
            dma((2,)),
            dma((zs - 1,)),
            dma((zs - 1,)),
            dma((2, zs - 1)),
            dma((2, zs - 1)),
            dma((1,)),
            dma((1,)),
            pltpu.SemaphoreType.REGULAR((max(zs - 2, 1),)),
        ],
        compiler_params=pltpu.CompilerParams(collective_id=0, has_side_effects=True),
    )(start, batches)
    result = pl.pallas_call(
        functools.partial(solve_kernel, rank, cols),
        out_shape=jax.ShapeDtypeStruct((rank, cols), f32),
        in_specs=[pl.BlockSpec(memory_space=pltpu.VMEM)] * 3,
        out_specs=pl.BlockSpec(memory_space=pl.ANY),
        scratch_shapes=[
            vm((hr, cols), jnp.bfloat16),
            vm((hr, cols), jnp.bfloat16),
            vm((rank, cols), f32),
            dma((2 * PIECES,)),
        ],
    )(
        pltpu.with_memory_space_constraint(gram, pltpu.VMEM),
        pltpu.with_memory_space_constraint(mh, pltpu.VMEM),
        pltpu.with_memory_space_constraint(ml, pltpu.VMEM),
    )
    return result[None]


def solution(mesh):
    placed = (P("rep", None, "feat"), P("rep", None, None, "feat"))
    return jax.shard_map(
        per_device, mesh=mesh, in_specs=placed, out_specs=P("rep", None, "feat"), check_vma=False
    )
```

```python
import functools

import jax
import jax.numpy as jnp
from jax import lax
from jax.experimental import pallas as pl
from jax.experimental.pallas import tpu as pltpu
from jax.sharding import PartitionSpec as P

learn_rate = 0.5
LANE = 128
PLAN = (2, 18, 3, 1)
SUB = 8
NB = 2
PIECES = 4
LATE = 2
MESH = pl.DeviceIdType.MESH
NN = (((1,), (0,)), ((), ()))
NT = (((1,), (1,)), ((), ()))


def exact_dot(left, right, dims):
    return lax.dot_general(
        left, right, dims, precision=lax.Precision.HIGHEST, preferred_element_type=jnp.float32
    )


def fast_dot(left, right, dims):
    return lax.dot_general(left, right, dims, preferred_element_type=jnp.float32)


def halves(value):
    high = value.astype(jnp.bfloat16)
    low = (value - high.astype(jnp.float32)).astype(jnp.bfloat16)
    return high, low


def gather_kernel(
    reps, feats, rank, rows, cols, total_feat,
    basis_hbm, stream_hbm, gram_ref, mh_ref, ml_ref,
    m_ref, w_ref, x_ref, whl_ref, sums_refs, recv_refs, av_ref,
    pay_ref, half_recv, half_sum, z_recv, full_ref,
    g_ref, g_recv,
    load_w, load_x_sem, ring_send, ring_recv, core_send, core_recv, z_send, z_recv_sem,
    g_send, g_recv_sem, hello_sem,
):
    bits = reps.bit_length() - 1
    chunk = LANE * reps
    chunks = cols // chunk
    zs = feats // 2
    me = lax.axis_index("rep")
    feat = lax.axis_index("feat")
    core = feat % 2
    zpos = feat // 2
    eta = learn_rate / rows
    scale = jnp.sqrt(jnp.float32(total_feat))

    def rep_peer(b):
        bit = (me // (1 << b)) % 2
        return me + (1 - 2 * bit) * (1 << b), bit

    rep_ids = [(rep_peer(b)[0], feat) for b in range(bits)]
    core_id = (me, feat + 1 - 2 * core)
    z_ids = [(me, ((zpos + d) % zs) * 2 + core) for d in range(1, zs)]

    beside = (zpos > 0).astype(jnp.int32) + (zpos < zs - 1).astype(jnp.int32)

    def tell_beside(sem):
        for ahead, there in ((-1, zpos > 0), (1, zpos < zs - 1)):

            @pl.when(there)
            def _():
                pl.semaphore_signal(
                    sem, inc=1, device_id=(me, feat + 2 * ahead), device_id_type=MESH
                )

    barrier = pltpu.get_barrier_semaphore()
    for peer in rep_ids + [core_id]:
        pl.semaphore_signal(barrier, inc=1, device_id=peer, device_id_type=MESH)
    tell_beside(barrier)
    load_basis = pltpu.make_async_copy(basis_hbm, w_ref, load_w)
    load_basis.start()
    load_x = pltpu.make_async_copy(stream_hbm, x_ref, load_x_sem)
    load_x.start()
    pl.semaphore_wait(barrier, bits + 1 + beside)

    def link(src, dst, send_sem, recv_sem, peer):
        return pltpu.make_async_remote_copy(
            src_ref=src, dst_ref=dst, send_sem=send_sem, recv_sem=recv_sem,
            device_id=peer, device_id_type=MESH,
        )

    def remote(*args):
        copy = link(*args)
        copy.start()
        return copy

    def at(off, width):
        return pl.ds(pl.multiple_of(off, LANE), width)

    def order(c):
        return [(c + i) % bits for i in range(bits)]

    keeps = []
    for c in range(chunks):
        off = c * chunk
        rec = []
        for i, b in enumerate(order(c)):
            width = chunk >> (i + 1)
            bit = rep_peer(b)[1]
            off = off + bit * width
            rec.append(off)
        keeps.append(rec)

    ring = {}

    def send_scatter(c, i):
        b = order(c)[i]
        width = chunk >> (i + 1)
        bit = rep_peer(b)[1]
        other = (1 - bit) * width
        if i == 0:
            src = w_ref.at[:, at(c * chunk + other, width)]
        else:
            src = sums_refs[i - 1].at[:, at(c * 2 * width + other, width)]
        dst = recv_refs[i].at[:, c * width:(c + 1) * width]
        ring[c, i] = remote(src, dst, ring_send.at[0], ring_recv.at[i, c], rep_ids[b])

    def take_scatter(c, i):
        b = order(c)[i]
        width = chunk >> (i + 1)
        bit = rep_peer(b)[1]
        ring[c, i].wait_recv()
        if i == 0:
            own = w_ref[:, at(c * chunk + bit * width, width)]
        else:
            own = sums_refs[i - 1][:, at(c * 2 * width + bit * width, width)]
        total = own + recv_refs[i][:, c * width:(c + 1) * width]
        if i == bits - 1:
            av_ref[:, at(keeps[c][i], width)] = total / reps
        else:
            sums_refs[i][:, c * width:(c + 1) * width] = total

    def send_gather(c, i):
        s = bits - 1 - i
        b = order(c)[s]
        width = chunk >> (s + 1)
        piece = av_ref.at[:, at(keeps[c][s], width)]
        k = bits + i
        ring[c, k] = remote(piece, piece, ring_send.at[1], ring_recv.at[k, c], rep_ids[b])

    load_basis.wait()
    for c in range(chunks):
        send_scatter(c, 0)
    rounds = zs - 2
    if rounds > 0:
        tell_beside(hello_sem.at[0])

    def step(c, i):
        if i < bits:
            take_scatter(c, i)
        else:
            ring[c, i].wait_recv()
        if i + 1 < bits:
            send_scatter(c, i + 1)
        elif i + 1 < 2 * bits:
            send_gather(c, i + 1 - bits)

    pending = [(c, i) for i in range(2 * bits - 1) for c in range(chunks)]
    place = [0]

    def advance(count):
        for _ in range(count):
            if place[0] < len(pending):
                step(*pending[place[0]])
                place[0] += 1

    high, low = halves(w_ref[...])
    whl_ref[0:rank, :] = high
    whl_ref[rank:2 * rank, :] = low
    load_x.wait()
    x_all = x_ref[...]
    wx = fast_dot(whl_ref[...], x_all, NT)
    wx = wx[0:rank] + wx[rank:2 * rank]
    pay_ref[0:rank, :] = wx[:, 0:rows]
    pay_ref[rank:2 * rank, :] = wx[:, rows:2 * rows]
    pay_ref[2 * rank:2 * rank + rows, :] = fast_dot(x_ref[0:rows, :], x_ref[rows:2 * rows, :], NT)

    half = rank + rows // 2
    give = pl.ds(pl.multiple_of((1 - core) * half, 8), half)
    keep = pl.ds(pl.multiple_of(core * half, 8), half)
    core_copy = remote(pay_ref.at[give, :], half_recv, core_send, core_recv.at[0], core_id)
    advance(PLAN[0])
    core_copy.wait_recv()
    half_sum[...] = pay_ref[keep, :] + half_recv[...]
    for k in range(rounds):
        pl.semaphore_wait(hello_sem.at[k], beside)
        if k + 1 < rounds:
            tell_beside(hello_sem.at[k + 1])
    for d in range(zs - 1):
        remote(half_sum, z_recv.at[d], z_send, z_recv_sem, z_ids[d])
    advance(PLAN[1])
    total = half_sum[...]
    z_all = link(z_recv, z_recv, z_send, z_recv_sem, core_id)
    z_all.wait_recv()
    for d in range(zs - 1):
        total = total + z_recv[d]
    full_ref[keep, :] = total
    share = remote(full_ref.at[keep, :], full_ref.at[keep, :], core_send, core_recv.at[1], core_id)
    advance(PLAN[2])
    share.wait_recv()

    first = full_ref[0:rank, :]
    second = full_ref[rank:2 * rank, :]
    cross = full_ref[2 * rank:2 * rank + rows, :]
    proj0 = first / scale
    cov0 = exact_dot(proj0, proj0, NT)
    drive1 = exact_dot(proj0, cross, NN)
    proj1 = (second + eta * (drive1 - exact_dot(cov0, second, NN))) / scale
    cov1 = exact_dot(proj1, proj1, NT)
    advance(PLAN[3])
    k_w = eta * (eta * exact_dot(cov1, cov0, NN) - cov0 - cov1)
    k_x0 = eta * (proj0 - eta * exact_dot(cov1, proj0, NN))
    k_x1 = eta * proj1
    kwh, kwl = halves(k_w)
    kx = jnp.concatenate([k_x0, k_x1], axis=1)
    kxh, kxl = halves(kx)
    kx2 = jnp.concatenate([kxh, kxl], axis=0)
    kw2 = jnp.concatenate([kwh, kwl], axis=0)

    def unmixed(c):
        cut = slice(c * chunk, (c + 1) * chunk)
        part = fast_dot(kx2, x_ref[:, cut], NN) + fast_dot(kw2, whl_ref[0:rank, cut], NN)
        part = part[0:rank] + part[rank:2 * rank] + fast_dot(kwh, whl_ref[rank:2 * rank, cut], NN)
        m_ref[:, cut] = part

    for c in range(chunks):
        unmixed(c)
        advance(1)
    advance(len(pending))

    slim = [jnp.zeros((2 * rank, rank), jnp.float32)]
    full = [jnp.zeros((rank, 2 * rank), jnp.float32)]

    def mix(off, width, late):
        cut = at(off, width)
        mh, ml = halves(m_ref[:, cut] + av_ref[:, cut])
        mh_ref[:, cut] = mh
        ml_ref[:, cut] = ml
        both = jnp.concatenate([mh, ml], axis=0)
        if late:
            part = fast_dot(both, jnp.concatenate([mh, mh], axis=0), NT)
            part = part[0:rank] + part[rank:2 * rank]
            full[0] = full[0] + (part + fast_dot(mh, jnp.concatenate([ml, ml], axis=0), NT))
        else:
            slim[0] = slim[0] + fast_dot(both, mh, NT)

    wide = chunk // 2
    for c in range(chunks):
        mix(keeps[c][0], wide, False)
    for c in range(chunks):
        if c == chunks - LATE:
            low_part = slim[0][rank:2 * rank]
            early = slim[0][0:rank] + (low_part + low_part.T)
            full[0] = full[0] + jnp.concatenate([early, early], axis=1)
        ring[c, 2 * bits - 1].wait_recv()
        mix(2 * c * chunk + wide - keeps[c][0], wide, c >= chunks - LATE)
    hr = rank // 2
    gram = full[0] * (1.0 / total_feat)
    lane = lax.broadcasted_iota(jnp.int32, (hr, 2 * rank), 1)
    g_ref[...] = jnp.where(lane < rank, gram[0:hr], gram[hr:rank])
    upper = (2 * zpos) // zs
    for j in range(zs - 1):
        far = upper * (j + (j >= zpos).astype(jnp.int32))
        near = (1 - upper) * (zs - 1 - j - (zs - 1 - j <= zpos).astype(jnp.int32))
        peer = far + near
        slot = (peer - zpos + zs) % zs - 1
        for k in range(2):
            remote(
                g_ref, g_recv.at[2 * slot + k], g_send, g_recv_sem,
                (me, peer * 2 + (core + k) % 2),
            )
    remote(g_ref, g_recv.at[2 * zs - 2], g_send, g_recv_sem, core_id)
    sent = cols - cols // reps
    g_all = link(g_recv, g_recv, g_send, g_recv_sem, core_id)
    link(w_ref.at[:, 0:sent], w_ref.at[:, 0:sent], ring_send.at[0], core_recv.at[0], core_id).wait_send()
    link(w_ref.at[:, 0:sent], w_ref.at[:, 0:sent], ring_send.at[1], core_recv.at[0], core_id).wait_send()
    link(pay_ref, pay_ref, core_send, core_recv.at[0], core_id).wait_send()
    z_all.wait_send()
    g_all.wait_send()
    g_all.wait_recv()
    total = g_ref[...]
    for d in range(2 * zs - 1):
        total = total + g_recv[d]
    gram_ref[...] = total


def lanes(block, lane):
    return jnp.broadcast_to(block[:, lane:lane + 1], block.shape)

def row(block, r):
    return jnp.broadcast_to(block[r:r + 1, :], block.shape)

def panel(blocks, first, nb, col, ids):
    w = SUB * nb
    last = len(blocks)
    own = [blocks[first + v] for v in range(nb)]
    keep = ids < w
    d = [[jnp.where(keep, lanes(own[v], col + k), 0.0) for v in range(nb)] for k in range(w)]
    c = {i: [lanes(blocks[i], col + k) for k in range(w)] for i in range(first + nb, last)}
    done = []
    for p in range(0, w, 2):
        v, s = divmod(p, SUB)
        a00, a10, a11 = row(d[p][v], s), row(d[p][v], s + 1), row(d[p + 1][v], s + 1)
        idet = 1.0 / (a00 * a11 - a10 * a10)
        i00, i01, i11 = a11 * idet, -(a10 * idet), a00 * idet
        at0, pair = ids == s, (ids == s) | (ids == s + 1)
        e0 = [d[p][u] * i00 + d[p + 1][u] * i01 for u in range(nb)]
        e1 = [d[p][u] * i01 + d[p + 1][u] * i11 for u in range(nb)]
        e0[v] = jnp.where(pair, jnp.where(at0, -i00, -i01), e0[v])
        e1[v] = jnp.where(pair, jnp.where(at0, -i01, -i11), e1[v])

        def step(x):
            t0, t1 = row(x[v], s), row(x[v], s + 1)
            base = [jnp.where(pair, 0.0, x[u]) if u == v else x[u] for u in range(nb)]
            return t0, t1, [base[u] - (e0[u] * t0 + e1[u] * t1) for u in range(nb)]

        r0, r1, own = step(own)
        ratio = a10 / a00
        done.append(r0 * lax.rsqrt(a00))
        done.append((r1 - ratio * r0) * lax.rsqrt(a11 - ratio * a10))
        for k in range(p + 2, w):
            d[k] = step(d[k])[2]
    if c:
        z = [row(own[p // SUB], p % SUB) for p in range(w)]
        for i in c:
            parts = [c[i][p] * z[p] for p in range(w)]
            while len(parts) > 1:
                parts = [parts[q] + parts[q + 1] for q in range(0, len(parts), 2)]
            blocks[i] = blocks[i] - parts[0]
    res = []
    for v in range(nb):
        out = done[v * SUB]
        for s in range(1, SUB):
            out = jnp.where(ids == s, done[v * SUB + s], out)
        res.append(out)
    return res
def solve_kernel(rank, cols, gram_ref, mh_ref, ml_ref, out_hbm, ph_ref, pl_ref, o_ref, out_sem):
    hr = rank // 2
    n = rank // SUB
    half = n // 2
    lane = lax.broadcasted_iota(jnp.int32, (SUB, 2 * rank), 1)
    ids = lax.broadcasted_iota(jnp.int32, (SUB, 2 * rank), 0)
    both = gram_ref[...]
    zero = jnp.zeros((SUB, rank), jnp.float32)
    top = [both[i * SUB:(i + 1) * SUB, :] for i in range(half)]
    low = [jnp.concatenate([t[:, rank:2 * rank], zero], axis=1) for t in top]
    blocks = [
        jnp.where(lane < rank, top[i], jnp.where(lane == rank + ids + i * SUB, 1.0, 0.0))
        for i in range(half)
    ] + low
    width = cols // PIECES

    def send(lo, p):
        cut = slice(p * width, (p + 1) * width)
        copy = pltpu.make_async_copy(
            o_ref.at[lo:lo + hr, cut], out_hbm.at[lo:lo + hr, cut], out_sem
        )
        copy.start()

    def eliminate(first):
        scaled = []
        for b in range(first, first + half, NB):
            scaled += panel(blocks, b, NB, b * SUB, ids)
        return scaled

    scaled = eliminate(0)
    left = jnp.concatenate(scaled + blocks[half:], axis=0)[:, rank:rank + hr]
    th, tl = halves(left)
    thl = jnp.concatenate([th, tl], axis=0)
    for p in range(PIECES):
        cut = slice(p * width, (p + 1) * width)
        part = fast_dot(thl, mh_ref[0:hr, cut], NN)
        part = part[0:rank] + part[rank:2 * rank] + fast_dot(th, ml_ref[0:hr, cut], NN)
        o_ref[0:hr, cut] = part[0:hr]
        send(0, p)
        rest = part[hr:rank] + mh_ref[hr:rank, cut].astype(jnp.float32)
        rest = rest + ml_ref[hr:rank, cut].astype(jnp.float32)
        ph_ref[:, cut], pl_ref[:, cut] = halves(rest)
    for i in range(half):
        unit = jnp.where(lane % hr == ids + i * SUB, 1.0, 0.0)
        pivots = (lane >= hr) & (lane < rank)
        blocks[half + i] = jnp.where(pivots, blocks[half + i], unit)
    left = jnp.concatenate(eliminate(half), axis=0)
    wide_lane = lax.broadcasted_iota(jnp.int32, (hr, 2 * rank), 1)
    left = jnp.where((wide_lane >= hr) & (wide_lane < rank), 0.0, left)
    th, tl = halves(left)
    low_lane = (wide_lane >= rank) & (wide_lane < rank + hr)
    mixed = jnp.where(low_lane, tl.astype(jnp.float32), th.astype(jnp.float32))
    mixed = mixed.astype(jnp.bfloat16)
    for p in range(PIECES):
        cut = slice(p * width, (p + 1) * width)
        ph, pl_ = ph_ref[:, cut], pl_ref[:, cut]
        o_ref[hr:rank, cut] = fast_dot(mixed, jnp.concatenate([ph, pl_, ph, pl_], axis=0), NN)
        send(hr, p)
    pltpu.make_async_copy(o_ref, out_hbm, out_sem).wait()


def per_device(basis, stream):
    reps = lax.axis_size("rep")
    feats = lax.axis_size("feat")
    start = basis[0]
    steps, rows, cols = stream.shape[1:]
    batches = stream[0].reshape(steps * rows, cols)
    rank = start.shape[0]
    bits = reps.bit_length() - 1
    chunk = LANE * reps
    chunks = cols // chunk
    zs = feats // 2
    half = rank + rows // 2
    f32 = jnp.float32
    vm = pltpu.VMEM
    hr = rank // 2
    dma = pltpu.SemaphoreType.DMA
    gram, mh, ml = pl.pallas_call(
        functools.partial(gather_kernel, reps, feats, rank, rows, cols, cols * feats),
        out_shape=(
            pltpu.VMEM((hr, 2 * rank), f32),
            pltpu.VMEM((rank, cols), jnp.bfloat16),
            pltpu.VMEM((rank, cols), jnp.bfloat16),
        ),
        in_specs=[pl.BlockSpec(memory_space=pl.ANY)] * 2,
        out_specs=(pl.BlockSpec(memory_space=pltpu.VMEM),) * 3,
        scratch_shapes=[
            vm((rank, cols), f32),
            vm((rank, cols), f32),
            vm((steps * rows, cols), jnp.bfloat16),
            vm((2 * rank, cols), jnp.bfloat16),
            [vm((rank, cols >> (i + 1)), f32) for i in range(bits)],
            [vm((rank, cols >> (i + 1)), f32) for i in range(bits)],
            vm((rank, cols), f32),
            vm((2 * half, rows), f32),
            vm((half, rows), f32),
            vm((half, rows), f32),
            vm((zs - 1, half, rows), f32),
            vm((2 * half, rows), f32),
            vm((hr, 2 * rank), f32),
            vm((2 * zs - 1, hr, 2 * rank), f32),
            dma,
            dma,
            dma((2,)),
            dma((2 * bits, chunks)),
            dma,
            dma((2,)),
            dma,
            dma,
            dma,
            dma,
            pltpu.SemaphoreType.REGULAR((max(zs - 2, 1),)),
        ],
        compiler_params=pltpu.CompilerParams(collective_id=0, has_side_effects=True),
    )(start, batches)
    result = pl.pallas_call(
        functools.partial(solve_kernel, rank, cols),
        out_shape=jax.ShapeDtypeStruct((rank, cols), f32),
        in_specs=[pl.BlockSpec(memory_space=pltpu.VMEM)] * 3,
        out_specs=pl.BlockSpec(memory_space=pl.ANY),
        scratch_shapes=[
            vm((hr, cols), jnp.bfloat16),
            vm((hr, cols), jnp.bfloat16),
            vm((rank, cols), f32),
            dma,
        ],
    )(
        pltpu.with_memory_space_constraint(gram, pltpu.VMEM),
        pltpu.with_memory_space_constraint(mh, pltpu.VMEM),
        pltpu.with_memory_space_constraint(ml, pltpu.VMEM),
    )
    return result[None]


def solution(mesh):
    placed = (P("rep", None, "feat"), P("rep", None, None, "feat"))
    return jax.shard_map(
        per_device, mesh=mesh, in_specs=placed, out_specs=P("rep", None, "feat"), check_vma=False
    )
```

```python
import functools

import jax
import jax.numpy as jnp
from jax import lax
from jax.experimental import pallas as pl
from jax.experimental.pallas import tpu as pltpu
from jax.sharding import PartitionSpec as P

learn_rate = 0.5
LANE = 128
PLAN = (2, 18, 3, 1)
SUB = 8
NB = 2
PIECES = 4
LATE = 2
MESH = pl.DeviceIdType.MESH
NN = (((1,), (0,)), ((), ()))
NT = (((1,), (1,)), ((), ()))


def exact_dot(left, right, dims):
    return lax.dot_general(
        left, right, dims, precision=lax.Precision.HIGHEST, preferred_element_type=jnp.float32
    )


def fast_dot(left, right, dims):
    return lax.dot_general(left, right, dims, preferred_element_type=jnp.float32)


def halves(value):
    high = value.astype(jnp.bfloat16)
    low = (value - high.astype(jnp.float32)).astype(jnp.bfloat16)
    return high, low


def gather_kernel(
    reps, feats, rank, rows, cols, total_feat,
    basis_hbm, stream_hbm, gram_ref, mh_ref, ml_ref,
    m_ref, w_ref, x_ref, whl_ref, sums_refs, recv_refs, av_ref,
    pay_ref, half_recv, half_sum, z_recv, full_ref,
    g_ref, g_recv,
    load_w, load_x_sem, ring_send, ring_recv, core_send, core_recv, z_send, z_recv_sem,
    g_send, g_recv_sem, hello_sem,
):
    bits = reps.bit_length() - 1
    chunk = LANE * reps
    chunks = cols // chunk
    zs = feats // 2
    me = lax.axis_index("rep")
    feat = lax.axis_index("feat")
    core = feat % 2
    zpos = feat // 2
    eta = learn_rate / rows
    scale = jnp.sqrt(jnp.float32(total_feat))

    def rep_peer(b):
        bit = (me // (1 << b)) % 2
        return me + (1 - 2 * bit) * (1 << b), bit

    rep_ids = [(rep_peer(b)[0], feat) for b in range(bits)]
    core_id = (me, feat + 1 - 2 * core)
    z_ids = [(me, ((zpos + d) % zs) * 2 + core) for d in range(1, zs)]

    beside = (zpos > 0).astype(jnp.int32) + (zpos < zs - 1).astype(jnp.int32)

    def tell_beside(sem):
        for ahead, there in ((-1, zpos > 0), (1, zpos < zs - 1)):

            @pl.when(there)
            def _():
                pl.semaphore_signal(
                    sem, inc=1, device_id=(me, feat + 2 * ahead), device_id_type=MESH
                )

    barrier = pltpu.get_barrier_semaphore()
    for peer in rep_ids + [core_id]:
        pl.semaphore_signal(barrier, inc=1, device_id=peer, device_id_type=MESH)
    tell_beside(barrier)
    load_basis = pltpu.make_async_copy(basis_hbm, w_ref, load_w)
    load_basis.start()
    load_x = pltpu.make_async_copy(stream_hbm, x_ref, load_x_sem)
    load_x.start()
    pl.semaphore_wait(barrier, bits + 1 + beside)

    def link(src, dst, send_sem, recv_sem, peer):
        return pltpu.make_async_remote_copy(
            src_ref=src, dst_ref=dst, send_sem=send_sem, recv_sem=recv_sem,
            device_id=peer, device_id_type=MESH,
        )

    def remote(*args):
        copy = link(*args)
        copy.start()
        return copy

    def at(off, width):
        return pl.ds(pl.multiple_of(off, LANE), width)

    def order(c):
        return [(c + i) % bits for i in range(bits)]

    keeps = []
    for c in range(chunks):
        off = c * chunk
        rec = []
        for i, b in enumerate(order(c)):
            width = chunk >> (i + 1)
            bit = rep_peer(b)[1]
            off = off + bit * width
            rec.append(off)
        keeps.append(rec)

    ring = {}

    def send_scatter(c, i):
        b = order(c)[i]
        width = chunk >> (i + 1)
        bit = rep_peer(b)[1]
        other = (1 - bit) * width
        if i == 0:
            src = w_ref.at[:, at(c * chunk + other, width)]
        else:
            src = sums_refs[i - 1].at[:, at(c * 2 * width + other, width)]
        dst = recv_refs[i].at[:, c * width:(c + 1) * width]
        ring[c, i] = remote(src, dst, ring_send.at[0], ring_recv.at[i, c], rep_ids[b])

    def take_scatter(c, i):
        b = order(c)[i]
        width = chunk >> (i + 1)
        bit = rep_peer(b)[1]
        ring[c, i].wait_recv()
        if i == 0:
            own = w_ref[:, at(c * chunk + bit * width, width)]
        else:
            own = sums_refs[i - 1][:, at(c * 2 * width + bit * width, width)]
        total = own + recv_refs[i][:, c * width:(c + 1) * width]
        if i == bits - 1:
            av_ref[:, at(keeps[c][i], width)] = total / reps
        else:
            sums_refs[i][:, c * width:(c + 1) * width] = total

    def send_gather(c, i):
        s = bits - 1 - i
        b = order(c)[s]
        width = chunk >> (s + 1)
        piece = av_ref.at[:, at(keeps[c][s], width)]
        k = bits + i
        ring[c, k] = remote(piece, piece, ring_send.at[1], ring_recv.at[k - 1 if i else 0, c], rep_ids[b])

    load_basis.wait()
    for c in range(chunks):
        send_scatter(c, 0)
    rounds = zs - 2
    if rounds > 0:
        tell_beside(hello_sem.at[0])

    def step(c, i):
        if i < bits:
            take_scatter(c, i)
        else:
            ring[c, i].wait_recv()
        if i + 1 < bits:
            send_scatter(c, i + 1)
        elif i + 1 < 2 * bits:
            send_gather(c, i + 1 - bits)

    pending = [(c, i) for i in range(2 * bits - 1) for c in range(chunks)]
    place = [0]

    def advance(count):
        for _ in range(count):
            if place[0] < len(pending):
                step(*pending[place[0]])
                place[0] += 1

    high, low = halves(w_ref[...])
    whl_ref[0:rank, :] = high
    whl_ref[rank:2 * rank, :] = low
    load_x.wait()
    x_all = x_ref[...]
    wx = fast_dot(whl_ref[...], x_all, NT)
    wx = wx[0:rank] + wx[rank:2 * rank]
    pay_ref[0:rank, :] = wx[:, 0:rows]
    pay_ref[rank:2 * rank, :] = wx[:, rows:2 * rows]
    pay_ref[2 * rank:2 * rank + rows, :] = fast_dot(x_ref[0:rows, :], x_ref[rows:2 * rows, :], NT)

    half = rank + rows // 2
    give = pl.ds(pl.multiple_of((1 - core) * half, 8), half)
    keep = pl.ds(pl.multiple_of(core * half, 8), half)
    core_copy = remote(pay_ref.at[give, :], half_recv, core_send, core_recv.at[0], core_id)
    advance(PLAN[0])
    core_copy.wait_recv()
    half_sum[...] = pay_ref[keep, :] + half_recv[...]
    for k in range(rounds):
        pl.semaphore_wait(hello_sem.at[k], beside)
        if k + 1 < rounds:
            tell_beside(hello_sem.at[k + 1])
    for d in range(zs - 1):
        remote(half_sum, z_recv.at[d], z_send, z_recv_sem, z_ids[d])
    advance(PLAN[1])
    total = half_sum[...]
    z_all = link(z_recv, z_recv, z_send, z_recv_sem, core_id)
    z_all.wait_recv()
    for d in range(zs - 1):
        total = total + z_recv[d]
    full_ref[keep, :] = total
    share = remote(full_ref.at[keep, :], full_ref.at[keep, :], core_send, core_recv.at[1], core_id)
    advance(PLAN[2])
    share.wait_recv()

    first = full_ref[0:rank, :]
    second = full_ref[rank:2 * rank, :]
    cross = full_ref[2 * rank:2 * rank + rows, :]
    proj0 = first / scale
    cov0 = exact_dot(proj0, proj0, NT)
    drive1 = exact_dot(proj0, cross, NN)
    proj1 = (second + eta * (drive1 - exact_dot(cov0, second, NN))) / scale
    cov1 = exact_dot(proj1, proj1, NT)
    advance(PLAN[3])
    k_w = eta * (eta * exact_dot(cov1, cov0, NN) - cov0 - cov1)
    k_x0 = eta * (proj0 - eta * exact_dot(cov1, proj0, NN))
    k_x1 = eta * proj1
    kwh, kwl = halves(k_w)
    kx = jnp.concatenate([k_x0, k_x1], axis=1)
    kxh, kxl = halves(kx)
    kx2 = jnp.concatenate([kxh, kxl], axis=0)
    kw2 = jnp.concatenate([kwh, kwl], axis=0)

    def unmixed(c):
        cut = slice(c * chunk, (c + 1) * chunk)
        part = fast_dot(kx2, x_ref[:, cut], NN) + fast_dot(kw2, whl_ref[0:rank, cut], NN)
        part = part[0:rank] + part[rank:2 * rank] + fast_dot(kwh, whl_ref[rank:2 * rank, cut], NN)
        m_ref[:, cut] = part

    for c in range(chunks):
        unmixed(c)
        advance(1)
    advance(len(pending))

    slim = [jnp.zeros((2 * rank, rank), jnp.float32)]
    full = [jnp.zeros((rank, 2 * rank), jnp.float32)]

    def mix(off, width, late):
        cut = at(off, width)
        mh, ml = halves(m_ref[:, cut] + av_ref[:, cut])
        mh_ref[:, cut] = mh
        ml_ref[:, cut] = ml
        both = jnp.concatenate([mh, ml], axis=0)
        if late:
            part = fast_dot(both, jnp.concatenate([mh, mh], axis=0), NT)
            part = part[0:rank] + part[rank:2 * rank]
            full[0] = full[0] + (part + fast_dot(mh, jnp.concatenate([ml, ml], axis=0), NT))
        else:
            slim[0] = slim[0] + fast_dot(both, mh, NT)

    wide = chunk // 2
    for c in range(chunks):
        mix(keeps[c][0], wide, False)
    for c in range(chunks):
        if c == chunks - LATE:
            low_part = slim[0][rank:2 * rank]
            early = slim[0][0:rank] + (low_part + low_part.T)
            full[0] = full[0] + jnp.concatenate([early, early], axis=1)
        ring[c, 2 * bits - 1].wait_recv()
        mix(2 * c * chunk + wide - keeps[c][0], wide, c >= chunks - LATE)
    hr = rank // 2
    gram = full[0] * (1.0 / total_feat)
    lane = lax.broadcasted_iota(jnp.int32, (hr, 2 * rank), 1)
    g_ref[...] = jnp.where(lane < rank, gram[0:hr], gram[hr:rank])
    upper = (2 * zpos) // zs
    for j in range(zs - 1):
        far = upper * (j + (j >= zpos).astype(jnp.int32))
        near = (1 - upper) * (zs - 1 - j - (zs - 1 - j <= zpos).astype(jnp.int32))
        peer = far + near
        slot = (peer - zpos + zs) % zs - 1
        for k in range(2):
            remote(
                g_ref, g_recv.at[2 * slot + k], g_send, g_recv_sem,
                (me, peer * 2 + (core + k) % 2),
            )
    remote(g_ref, g_recv.at[2 * zs - 2], g_send, g_recv_sem, core_id)
    sent = cols - cols // reps
    g_all = link(g_recv, g_recv, g_send, g_recv_sem, core_id)
    link(w_ref.at[:, 0:sent], w_ref.at[:, 0:sent], ring_send.at[0], core_recv.at[0], core_id).wait_send()
    link(w_ref.at[:, 0:sent], w_ref.at[:, 0:sent], ring_send.at[1], core_recv.at[0], core_id).wait_send()
    link(pay_ref, pay_ref, core_send, core_recv.at[0], core_id).wait_send()
    z_all.wait_send()
    g_all.wait_send()
    g_all.wait_recv()
    total = g_ref[...]
    for d in range(2 * zs - 1):
        total = total + g_recv[d]
    gram_ref[...] = total


def lanes(block, lane):
    return jnp.broadcast_to(block[:, lane:lane + 1], block.shape)

def row(block, r):
    return jnp.broadcast_to(block[r:r + 1, :], block.shape)

def panel(blocks, first, nb, col, ids):
    w = SUB * nb
    last = len(blocks)
    own = [blocks[first + v] for v in range(nb)]
    keep = ids < w
    d = [[jnp.where(keep, lanes(own[v], col + k), 0.0) for v in range(nb)] for k in range(w)]
    c = {i: [lanes(blocks[i], col + k) for k in range(w)] for i in range(first + nb, last)}
    done = []
    for p in range(0, w, 2):
        v, s = divmod(p, SUB)
        a00, a10, a11 = row(d[p][v], s), row(d[p][v], s + 1), row(d[p + 1][v], s + 1)
        idet = 1.0 / (a00 * a11 - a10 * a10)
        i00, i01, i11 = a11 * idet, -(a10 * idet), a00 * idet
        at0, pair = ids == s, (ids == s) | (ids == s + 1)
        e0 = [d[p][u] * i00 + d[p + 1][u] * i01 for u in range(nb)]
        e1 = [d[p][u] * i01 + d[p + 1][u] * i11 for u in range(nb)]
        e0[v] = jnp.where(pair, jnp.where(at0, -i00, -i01), e0[v])
        e1[v] = jnp.where(pair, jnp.where(at0, -i01, -i11), e1[v])

        def step(x):
            t0, t1 = row(x[v], s), row(x[v], s + 1)
            base = [jnp.where(pair, 0.0, x[u]) if u == v else x[u] for u in range(nb)]
            return t0, t1, [base[u] - (e0[u] * t0 + e1[u] * t1) for u in range(nb)]

        r0, r1, own = step(own)
        ratio = a10 / a00
        done.append(r0 * lax.rsqrt(a00))
        done.append((r1 - ratio * r0) * lax.rsqrt(a11 - ratio * a10))
        for k in range(p + 2, w):
            d[k] = step(d[k])[2]
    if c:
        z = [row(own[p // SUB], p % SUB) for p in range(w)]
        for i in c:
            parts = [c[i][p] * z[p] for p in range(w)]
            while len(parts) > 1:
                parts = [parts[q] + parts[q + 1] for q in range(0, len(parts), 2)]
            blocks[i] = blocks[i] - parts[0]
    res = []
    for v in range(nb):
        out = done[v * SUB]
        for s in range(1, SUB):
            out = jnp.where(ids == s, done[v * SUB + s], out)
        res.append(out)
    return res
def solve_kernel(rank, cols, gram_ref, mh_ref, ml_ref, out_hbm, ph_ref, pl_ref, o_ref, out_sem):
    hr = rank // 2
    n = rank // SUB
    half = n // 2
    lane = lax.broadcasted_iota(jnp.int32, (SUB, 2 * rank), 1)
    ids = lax.broadcasted_iota(jnp.int32, (SUB, 2 * rank), 0)
    both = gram_ref[...]
    zero = jnp.zeros((SUB, rank), jnp.float32)
    top = [both[i * SUB:(i + 1) * SUB, :] for i in range(half)]
    low = [jnp.concatenate([t[:, rank:2 * rank], zero], axis=1) for t in top]
    blocks = [
        jnp.where(lane < rank, top[i], jnp.where(lane == rank + ids + i * SUB, 1.0, 0.0))
        for i in range(half)
    ] + low
    width = cols // PIECES

    def send(lo, p):
        cut = slice(p * width, (p + 1) * width)
        copy = pltpu.make_async_copy(
            o_ref.at[lo:lo + hr, cut], out_hbm.at[lo:lo + hr, cut], out_sem
        )
        copy.start()

    def eliminate(first):
        scaled = []
        for b in range(first, first + half, NB):
            scaled += panel(blocks, b, NB, b * SUB, ids)
        return scaled

    scaled = eliminate(0)
    left = jnp.concatenate(scaled + blocks[half:], axis=0)[:, rank:rank + hr]
    th, tl = halves(left)
    thl = jnp.concatenate([th, tl], axis=0)
    for p in range(PIECES):
        cut = slice(p * width, (p + 1) * width)
        part = fast_dot(thl, mh_ref[0:hr, cut], NN)
        part = part[0:rank] + part[rank:2 * rank] + fast_dot(th, ml_ref[0:hr, cut], NN)
        o_ref[0:hr, cut] = part[0:hr]
        send(0, p)
        rest = part[hr:rank] + mh_ref[hr:rank, cut].astype(jnp.float32)
        rest = rest + ml_ref[hr:rank, cut].astype(jnp.float32)
        ph_ref[:, cut], pl_ref[:, cut] = halves(rest)
    for i in range(half):
        unit = jnp.where(lane % hr == ids + i * SUB, 1.0, 0.0)
        pivots = (lane >= hr) & (lane < rank)
        blocks[half + i] = jnp.where(pivots, blocks[half + i], unit)
    left = jnp.concatenate(eliminate(half), axis=0)
    wide_lane = lax.broadcasted_iota(jnp.int32, (hr, 2 * rank), 1)
    left = jnp.where((wide_lane >= hr) & (wide_lane < rank), 0.0, left)
    th, tl = halves(left)
    low_lane = (wide_lane >= rank) & (wide_lane < rank + hr)
    mixed = jnp.where(low_lane, tl.astype(jnp.float32), th.astype(jnp.float32))
    mixed = mixed.astype(jnp.bfloat16)
    for p in range(PIECES):
        cut = slice(p * width, (p + 1) * width)
        ph, pl_ = ph_ref[:, cut], pl_ref[:, cut]
        o_ref[hr:rank, cut] = fast_dot(mixed, jnp.concatenate([ph, pl_, ph, pl_], axis=0), NN)
        send(hr, p)
    pltpu.make_async_copy(o_ref, out_hbm, out_sem).wait()


def per_device(basis, stream):
    reps = lax.axis_size("rep")
    feats = lax.axis_size("feat")
    start = basis[0]
    steps, rows, cols = stream.shape[1:]
    batches = stream[0].reshape(steps * rows, cols)
    rank = start.shape[0]
    bits = reps.bit_length() - 1
    chunk = LANE * reps
    chunks = cols // chunk
    zs = feats // 2
    half = rank + rows // 2
    f32 = jnp.float32
    vm = pltpu.VMEM
    hr = rank // 2
    dma = pltpu.SemaphoreType.DMA
    gram, mh, ml = pl.pallas_call(
        functools.partial(gather_kernel, reps, feats, rank, rows, cols, cols * feats),
        out_shape=(
            pltpu.VMEM((hr, 2 * rank), f32),
            pltpu.VMEM((rank, cols), jnp.bfloat16),
            pltpu.VMEM((rank, cols), jnp.bfloat16),
        ),
        in_specs=[pl.BlockSpec(memory_space=pl.ANY)] * 2,
        out_specs=(pl.BlockSpec(memory_space=pltpu.VMEM),) * 3,
        scratch_shapes=[
            vm((rank, cols), f32),
            vm((rank, cols), f32),
            vm((steps * rows, cols), jnp.bfloat16),
            vm((2 * rank, cols), jnp.bfloat16),
            [vm((rank, cols >> (i + 1)), f32) for i in range(bits)],
            [vm((rank, cols >> (i + 1)), f32) for i in range(bits)],
            vm((rank, cols), f32),
            vm((2 * half, rows), f32),
            vm((half, rows), f32),
            vm((half, rows), f32),
            vm((zs - 1, half, rows), f32),
            vm((2 * half, rows), f32),
            vm((hr, 2 * rank), f32),
            vm((2 * zs - 1, hr, 2 * rank), f32),
            dma,
            dma,
            dma((2,)),
            dma((2 * bits - 1, chunks)),
            dma,
            dma((2,)),
            dma,
            dma,
            dma,
            dma,
            pltpu.SemaphoreType.REGULAR((max(zs - 2, 1),)),
        ],
        compiler_params=pltpu.CompilerParams(collective_id=0, has_side_effects=True),
    )(start, batches)
    result = pl.pallas_call(
        functools.partial(solve_kernel, rank, cols),
        out_shape=jax.ShapeDtypeStruct((rank, cols), f32),
        in_specs=[pl.BlockSpec(memory_space=pltpu.VMEM)] * 3,
        out_specs=pl.BlockSpec(memory_space=pl.ANY),
        scratch_shapes=[
            vm((hr, cols), jnp.bfloat16),
            vm((hr, cols), jnp.bfloat16),
            vm((rank, cols), f32),
            dma,
        ],
    )(
        pltpu.with_memory_space_constraint(gram, pltpu.VMEM),
        pltpu.with_memory_space_constraint(mh, pltpu.VMEM),
        pltpu.with_memory_space_constraint(ml, pltpu.VMEM),
    )
    return result[None]


def solution(mesh):
    placed = (P("rep", None, "feat"), P("rep", None, None, "feat"))
    return jax.shard_map(
        per_device, mesh=mesh, in_specs=placed, out_specs=P("rep", None, "feat"), check_vma=False
    )
```

```python
import functools

import jax
import jax.numpy as jnp
from jax import lax
from jax.experimental import pallas as pl
from jax.experimental.pallas import tpu as pltpu
from jax.sharding import PartitionSpec as P

learn_rate = 0.5
LANE = 128
PLAN = (2, 18, 3, 1)
SUB = 8
NB = 2
PIECES = 4
LATE = 2
MESH = pl.DeviceIdType.MESH
NN = (((1,), (0,)), ((), ()))
NT = (((1,), (1,)), ((), ()))


def exact_dot(left, right, dims):
    return lax.dot_general(
        left, right, dims, precision=lax.Precision.HIGHEST, preferred_element_type=jnp.float32
    )


def fast_dot(left, right, dims):
    return lax.dot_general(left, right, dims, preferred_element_type=jnp.float32)


def halves(value):
    high = value.astype(jnp.bfloat16)
    low = (value - high.astype(jnp.float32)).astype(jnp.bfloat16)
    return high, low


def gather_kernel(
    reps, feats, rank, rows, cols, total_feat,
    basis_hbm, stream_hbm, gram_ref, mh_ref, ml_ref,
    m_ref, w_ref, x_ref, whl_ref, sums_refs, recv_refs, av_ref,
    pay_ref, half_recv, half_sum, z_recv, full_ref,
    g_ref, g_recv,
    load_f, load_w, load_x_sem, ring_send, ring_recv, more_recv, core_send, core_recv, z_send, z_recv_sem,
    g_send, g_recv_sem, hello_sem,
):
    bits = reps.bit_length() - 1
    chunk = LANE * reps
    chunks = cols // chunk
    zs = feats // 2
    me = lax.axis_index("rep")
    feat = lax.axis_index("feat")
    core = feat % 2
    zpos = feat // 2
    eta = learn_rate / rows
    scale = jnp.sqrt(jnp.float32(total_feat))

    def rep_peer(b):
        bit = (me // (1 << b)) % 2
        return me + (1 - 2 * bit) * (1 << b), bit

    rep_ids = [(rep_peer(b)[0], feat) for b in range(bits)]
    core_id = (me, feat + 1 - 2 * core)
    z_ids = [(me, ((zpos + d) % zs) * 2 + core) for d in range(1, zs)]

    beside = (zpos > 0).astype(jnp.int32) + (zpos < zs - 1).astype(jnp.int32)

    def tell_beside(sem):
        for ahead, there in ((-1, zpos > 0), (1, zpos < zs - 1)):

            @pl.when(there)
            def _():
                pl.semaphore_signal(
                    sem, inc=1, device_id=(me, feat + 2 * ahead), device_id_type=MESH
                )

    barrier = pltpu.get_barrier_semaphore()
    for peer in rep_ids + [core_id]:
        pl.semaphore_signal(barrier, inc=1, device_id=peer, device_id_type=MESH)
    tell_beside(barrier)
    front = chunk * (chunks // 4)
    load_front = pltpu.make_async_copy(basis_hbm.at[:, 0:front], w_ref.at[:, 0:front], load_f)
    load_front.start()
    load_basis = pltpu.make_async_copy(basis_hbm.at[:, front:cols], w_ref.at[:, front:cols], load_w)
    load_basis.start()
    load_x = pltpu.make_async_copy(stream_hbm, x_ref, load_x_sem)
    load_x.start()
    pl.semaphore_wait(barrier, bits + 1 + beside)

    def link(src, dst, send_sem, recv_sem, peer):
        return pltpu.make_async_remote_copy(
            src_ref=src, dst_ref=dst, send_sem=send_sem, recv_sem=recv_sem,
            device_id=peer, device_id_type=MESH,
        )

    def remote(*args):
        copy = link(*args)
        copy.start()
        return copy

    def at(off, width):
        return pl.ds(pl.multiple_of(off, LANE), width)

    def order(c):
        return [(c + i) % bits for i in range(bits)]

    keeps = []
    for c in range(chunks):
        off = c * chunk
        rec = []
        for i, b in enumerate(order(c)):
            width = chunk >> (i + 1)
            bit = rep_peer(b)[1]
            off = off + bit * width
            rec.append(off)
        keeps.append(rec)

    ring = {}

    def send_scatter(c, i):
        b = order(c)[i]
        width = chunk >> (i + 1)
        bit = rep_peer(b)[1]
        other = (1 - bit) * width
        if i == 0:
            src = w_ref.at[:, at(c * chunk + other, width)]
        else:
            src = sums_refs[i - 1].at[:, at(c * 2 * width + other, width)]
        dst = recv_refs[i].at[:, c * width:(c + 1) * width]
        ring[c, i] = remote(src, dst, ring_send.at[0], ring_recv.at[i, c], rep_ids[b])

    def take_scatter(c, i):
        b = order(c)[i]
        width = chunk >> (i + 1)
        bit = rep_peer(b)[1]
        ring[c, i].wait_recv()
        if i == 0:
            own = w_ref[:, at(c * chunk + bit * width, width)]
        else:
            own = sums_refs[i - 1][:, at(c * 2 * width + bit * width, width)]
        total = own + recv_refs[i][:, c * width:(c + 1) * width]
        if i == bits - 1:
            av_ref[:, at(keeps[c][i], width)] = total / reps
        else:
            sums_refs[i][:, c * width:(c + 1) * width] = total

    def send_gather(c, i):
        s = bits - 1 - i
        b = order(c)[s]
        width = chunk >> (s + 1)
        piece = av_ref.at[:, at(keeps[c][s], width)]
        k = bits + i
        if i == 0:
            done = ring_recv.at[0, c]
        elif bits == 2 and c > 0:
            done = ring_recv.at[1, c - 1]
        else:
            done = more_recv.at[i - 1, c]
        ring[c, k] = remote(piece, piece, ring_send.at[1], done, rep_ids[b])

    load_front.wait()
    for c in range(chunks):
        if c == chunks // 4:
            load_basis.wait()
        send_scatter(c, 0)
    rounds = zs - 2
    if rounds > 0:
        tell_beside(hello_sem.at[0])

    def step(c, i):
        if i < bits:
            take_scatter(c, i)
        else:
            ring[c, i].wait_recv()
        if i + 1 < bits:
            send_scatter(c, i + 1)
        elif i + 1 < 2 * bits:
            send_gather(c, i + 1 - bits)

    pending = [(c, i) for i in range(2 * bits - 1) for c in range(chunks)]
    place = [0]

    def advance(count):
        for _ in range(count):
            if place[0] < len(pending):
                step(*pending[place[0]])
                place[0] += 1

    high, low = halves(w_ref[...])
    whl_ref[0:rank, :] = high
    whl_ref[rank:2 * rank, :] = low
    load_x.wait()
    x_all = x_ref[...]
    wx = fast_dot(whl_ref[...], x_all, NT)
    wx = wx[0:rank] + wx[rank:2 * rank]
    pay_ref[0:rank, :] = wx[:, 0:rows]
    pay_ref[rank:2 * rank, :] = wx[:, rows:2 * rows]
    pay_ref[2 * rank:2 * rank + rows, :] = fast_dot(x_ref[0:rows, :], x_ref[rows:2 * rows, :], NT)

    half = rank + rows // 2
    give = pl.ds(pl.multiple_of((1 - core) * half, 8), half)
    keep = pl.ds(pl.multiple_of(core * half, 8), half)
    core_copy = remote(pay_ref.at[give, :], half_recv, core_send, core_recv.at[0], core_id)
    advance(PLAN[0])
    core_copy.wait_recv()
    half_sum[...] = pay_ref[keep, :] + half_recv[...]
    for k in range(rounds):
        pl.semaphore_wait(hello_sem.at[k], beside)
        if k + 1 < rounds:
            tell_beside(hello_sem.at[k + 1])
    for d in range(zs - 1):
        remote(half_sum, z_recv.at[d], z_send, z_recv_sem, z_ids[d])
    advance(PLAN[1])
    total = half_sum[...]
    z_all = link(z_recv, z_recv, z_send, z_recv_sem, core_id)
    z_all.wait_recv()
    for d in range(zs - 1):
        total = total + z_recv[d]
    full_ref[keep, :] = total
    share = remote(full_ref.at[keep, :], full_ref.at[keep, :], core_send, core_recv.at[1], core_id)
    advance(PLAN[2])
    share.wait_recv()

    first = full_ref[0:rank, :]
    second = full_ref[rank:2 * rank, :]
    cross = full_ref[2 * rank:2 * rank + rows, :]
    proj0 = first / scale
    cov0 = exact_dot(proj0, proj0, NT)
    drive1 = exact_dot(proj0, cross, NN)
    proj1 = (second + eta * (drive1 - exact_dot(cov0, second, NN))) / scale
    cov1 = exact_dot(proj1, proj1, NT)
    advance(PLAN[3])
    k_w = eta * (eta * exact_dot(cov1, cov0, NN) - cov0 - cov1)
    k_x0 = eta * (proj0 - eta * exact_dot(cov1, proj0, NN))
    k_x1 = eta * proj1
    kwh, kwl = halves(k_w)
    kx = jnp.concatenate([k_x0, k_x1], axis=1)
    kxh, kxl = halves(kx)
    kx2 = jnp.concatenate([kxh, kxl], axis=0)
    kw2 = jnp.concatenate([kwh, kwl], axis=0)

    def unmixed(c):
        cut = slice(c * chunk, (c + 1) * chunk)
        part = fast_dot(kx2, x_ref[:, cut], NN) + fast_dot(kw2, whl_ref[0:rank, cut], NN)
        part = part[0:rank] + part[rank:2 * rank] + fast_dot(kwh, whl_ref[rank:2 * rank, cut], NN)
        m_ref[:, cut] = part

    for c in range(chunks):
        unmixed(c)
        advance(1)
    advance(len(pending))

    slim = [jnp.zeros((2 * rank, rank), jnp.float32)]
    full = [jnp.zeros((rank, 2 * rank), jnp.float32)]

    def mix(off, width, late):
        cut = at(off, width)
        mh, ml = halves(m_ref[:, cut] + av_ref[:, cut])
        mh_ref[:, cut] = mh
        ml_ref[:, cut] = ml
        both = jnp.concatenate([mh, ml], axis=0)
        if late:
            part = fast_dot(both, jnp.concatenate([mh, mh], axis=0), NT)
            part = part[0:rank] + part[rank:2 * rank]
            full[0] = full[0] + (part + fast_dot(mh, jnp.concatenate([ml, ml], axis=0), NT))
        else:
            slim[0] = slim[0] + fast_dot(both, mh, NT)

    wide = chunk // 2
    for c in range(chunks):
        mix(keeps[c][0], wide, False)
    for c in range(chunks):
        if c == chunks - LATE:
            low_part = slim[0][rank:2 * rank]
            early = slim[0][0:rank] + (low_part + low_part.T)
            full[0] = full[0] + jnp.concatenate([early, early], axis=1)
        ring[c, 2 * bits - 1].wait_recv()
        mix(2 * c * chunk + wide - keeps[c][0], wide, c >= chunks - LATE)
    hr = rank // 2
    gram = full[0] * (1.0 / total_feat)
    lane = lax.broadcasted_iota(jnp.int32, (hr, 2 * rank), 1)
    g_ref[...] = jnp.where(lane < rank, gram[0:hr], gram[hr:rank])
    upper = (2 * zpos) // zs
    for j in range(zs - 1):
        far = upper * (j + (j >= zpos).astype(jnp.int32))
        near = (1 - upper) * (zs - 1 - j - (zs - 1 - j <= zpos).astype(jnp.int32))
        peer = far + near
        slot = (peer - zpos + zs) % zs - 1
        for k in range(2):
            remote(
                g_ref, g_recv.at[2 * slot + k], g_send, g_recv_sem,
                (me, peer * 2 + (core + k) % 2),
            )
    remote(g_ref, g_recv.at[2 * zs - 2], g_send, g_recv_sem, core_id)
    sent = cols - cols // reps
    g_all = link(g_recv, g_recv, g_send, g_recv_sem, core_id)
    link(w_ref.at[:, 0:sent], w_ref.at[:, 0:sent], ring_send.at[0], core_recv.at[0], core_id).wait_send()
    link(w_ref.at[:, 0:sent], w_ref.at[:, 0:sent], ring_send.at[1], core_recv.at[0], core_id).wait_send()
    link(pay_ref, pay_ref, core_send, core_recv.at[0], core_id).wait_send()
    z_all.wait_send()
    g_all.wait_send()
    g_all.wait_recv()
    total = g_ref[...]
    for d in range(2 * zs - 1):
        total = total + g_recv[d]
    gram_ref[...] = total


def lanes(block, lane):
    return jnp.broadcast_to(block[:, lane:lane + 1], block.shape)

def row(block, r):
    return jnp.broadcast_to(block[r:r + 1, :], block.shape)

def panel(blocks, first, nb, col, ids):
    w = SUB * nb
    last = len(blocks)
    own = [blocks[first + v] for v in range(nb)]
    keep = ids < w
    d = [[jnp.where(keep, lanes(own[v], col + k), 0.0) for v in range(nb)] for k in range(w)]
    c = {i: [lanes(blocks[i], col + k) for k in range(w)] for i in range(first + nb, last)}
    done = []
    for p in range(0, w, 2):
        v, s = divmod(p, SUB)
        a00, a10, a11 = row(d[p][v], s), row(d[p][v], s + 1), row(d[p + 1][v], s + 1)
        idet = 1.0 / (a00 * a11 - a10 * a10)
        i00, i01, i11 = a11 * idet, -(a10 * idet), a00 * idet
        at0, pair = ids == s, (ids == s) | (ids == s + 1)
        e0 = [d[p][u] * i00 + d[p + 1][u] * i01 for u in range(nb)]
        e1 = [d[p][u] * i01 + d[p + 1][u] * i11 for u in range(nb)]
        e0[v] = jnp.where(pair, jnp.where(at0, -i00, -i01), e0[v])
        e1[v] = jnp.where(pair, jnp.where(at0, -i01, -i11), e1[v])

        def step(x):
            t0, t1 = row(x[v], s), row(x[v], s + 1)
            base = [jnp.where(pair, 0.0, x[u]) if u == v else x[u] for u in range(nb)]
            return t0, t1, [base[u] - (e0[u] * t0 + e1[u] * t1) for u in range(nb)]

        r0, r1, own = step(own)
        ratio = a10 / a00
        done.append(r0 * lax.rsqrt(a00))
        done.append((r1 - ratio * r0) * lax.rsqrt(a11 - ratio * a10))
        for k in range(p + 2, w):
            d[k] = step(d[k])[2]
    if c:
        z = [row(own[p // SUB], p % SUB) for p in range(w)]
        for i in c:
            parts = [c[i][p] * z[p] for p in range(w)]
            while len(parts) > 1:
                parts = [parts[q] + parts[q + 1] for q in range(0, len(parts), 2)]
            blocks[i] = blocks[i] - parts[0]
    res = []
    for v in range(nb):
        out = done[v * SUB]
        for s in range(1, SUB):
            out = jnp.where(ids == s, done[v * SUB + s], out)
        res.append(out)
    return res
def solve_kernel(rank, cols, gram_ref, mh_ref, ml_ref, out_hbm, ph_ref, pl_ref, o_ref, out_sem):
    hr = rank // 2
    n = rank // SUB
    half = n // 2
    lane = lax.broadcasted_iota(jnp.int32, (SUB, 2 * rank), 1)
    ids = lax.broadcasted_iota(jnp.int32, (SUB, 2 * rank), 0)
    both = gram_ref[...]
    zero = jnp.zeros((SUB, rank), jnp.float32)
    top = [both[i * SUB:(i + 1) * SUB, :] for i in range(half)]
    low = [jnp.concatenate([t[:, rank:2 * rank], zero], axis=1) for t in top]
    blocks = [
        jnp.where(lane < rank, top[i], jnp.where(lane == rank + ids + i * SUB, 1.0, 0.0))
        for i in range(half)
    ] + low
    width = cols // PIECES

    def send(lo, p):
        cut = slice(p * width, (p + 1) * width)
        copy = pltpu.make_async_copy(
            o_ref.at[lo:lo + hr, cut], out_hbm.at[lo:lo + hr, cut], out_sem
        )
        copy.start()

    def eliminate(first):
        scaled = []
        for b in range(first, first + half, NB):
            scaled += panel(blocks, b, NB, b * SUB, ids)
        return scaled

    scaled = eliminate(0)
    left = jnp.concatenate(scaled + blocks[half:], axis=0)[:, rank:rank + hr]
    th, tl = halves(left)
    thl = jnp.concatenate([th, tl], axis=0)
    for p in range(PIECES):
        cut = slice(p * width, (p + 1) * width)
        part = fast_dot(thl, mh_ref[0:hr, cut], NN)
        part = part[0:rank] + part[rank:2 * rank] + fast_dot(th, ml_ref[0:hr, cut], NN)
        o_ref[0:hr, cut] = part[0:hr]
        send(0, p)
        rest = part[hr:rank] + mh_ref[hr:rank, cut].astype(jnp.float32)
        rest = rest + ml_ref[hr:rank, cut].astype(jnp.float32)
        ph_ref[:, cut], pl_ref[:, cut] = halves(rest)
    for i in range(half):
        unit = jnp.where(lane % hr == ids + i * SUB, 1.0, 0.0)
        pivots = (lane >= hr) & (lane < rank)
        blocks[half + i] = jnp.where(pivots, blocks[half + i], unit)
    left = jnp.concatenate(eliminate(half), axis=0)
    wide_lane = lax.broadcasted_iota(jnp.int32, (hr, 2 * rank), 1)
    left = jnp.where((wide_lane >= hr) & (wide_lane < rank), 0.0, left)
    th, tl = halves(left)
    low_lane = (wide_lane >= rank) & (wide_lane < rank + hr)
    mixed = jnp.where(low_lane, tl.astype(jnp.float32), th.astype(jnp.float32))
    mixed = mixed.astype(jnp.bfloat16)
    for p in range(PIECES):
        cut = slice(p * width, (p + 1) * width)
        ph, pl_ = ph_ref[:, cut], pl_ref[:, cut]
        o_ref[hr:rank, cut] = fast_dot(mixed, jnp.concatenate([ph, pl_, ph, pl_], axis=0), NN)
        send(hr, p)
    pltpu.make_async_copy(o_ref, out_hbm, out_sem).wait()


def per_device(basis, stream):
    reps = lax.axis_size("rep")
    feats = lax.axis_size("feat")
    start = basis[0]
    steps, rows, cols = stream.shape[1:]
    batches = stream[0].reshape(steps * rows, cols)
    rank = start.shape[0]
    bits = reps.bit_length() - 1
    chunk = LANE * reps
    chunks = cols // chunk
    zs = feats // 2
    half = rank + rows // 2
    f32 = jnp.float32
    vm = pltpu.VMEM
    hr = rank // 2
    dma = pltpu.SemaphoreType.DMA
    gram, mh, ml = pl.pallas_call(
        functools.partial(gather_kernel, reps, feats, rank, rows, cols, cols * feats),
        out_shape=(
            pltpu.VMEM((hr, 2 * rank), f32),
            pltpu.VMEM((rank, cols), jnp.bfloat16),
            pltpu.VMEM((rank, cols), jnp.bfloat16),
        ),
        in_specs=[pl.BlockSpec(memory_space=pl.ANY)] * 2,
        out_specs=(pl.BlockSpec(memory_space=pltpu.VMEM),) * 3,
        scratch_shapes=[
            vm((rank, cols), f32),
            vm((rank, cols), f32),
            vm((steps * rows, cols), jnp.bfloat16),
            vm((2 * rank, cols), jnp.bfloat16),
            [vm((rank, cols >> (i + 1)), f32) for i in range(bits)],
            [vm((rank, cols >> (i + 1)), f32) for i in range(bits)],
            vm((rank, cols), f32),
            vm((2 * half, rows), f32),
            vm((half, rows), f32),
            vm((half, rows), f32),
            vm((zs - 1, half, rows), f32),
            vm((2 * half, rows), f32),
            vm((hr, 2 * rank), f32),
            vm((2 * zs - 1, hr, 2 * rank), f32),
            dma,
            dma,
            dma,
            dma((2,)),
            dma((bits, chunks)),
            dma((1, 1)) if bits == 2 else dma((bits - 1, chunks)),
            dma,
            dma((2,)),
            dma,
            dma,
            dma,
            dma,
            pltpu.SemaphoreType.REGULAR((max(zs - 2, 1),)),
        ],
        compiler_params=pltpu.CompilerParams(collective_id=0, has_side_effects=True),
    )(start, batches)
    result = pl.pallas_call(
        functools.partial(solve_kernel, rank, cols),
        out_shape=jax.ShapeDtypeStruct((rank, cols), f32),
        in_specs=[pl.BlockSpec(memory_space=pltpu.VMEM)] * 3,
        out_specs=pl.BlockSpec(memory_space=pl.ANY),
        scratch_shapes=[
            vm((hr, cols), jnp.bfloat16),
            vm((hr, cols), jnp.bfloat16),
            vm((rank, cols), f32),
            dma,
        ],
    )(
        pltpu.with_memory_space_constraint(gram, pltpu.VMEM),
        pltpu.with_memory_space_constraint(mh, pltpu.VMEM),
        pltpu.with_memory_space_constraint(ml, pltpu.VMEM),
    )
    return result[None]


def solution(mesh):
    placed = (P("rep", None, "feat"), P("rep", None, None, "feat"))
    return jax.shard_map(
        per_device, mesh=mesh, in_specs=placed, out_specs=P("rep", None, "feat"), check_vma=False
    )
```

```python
import functools

import jax
import jax.numpy as jnp
from jax import lax
from jax.experimental import pallas as pl
from jax.experimental.pallas import tpu as pltpu
from jax.sharding import PartitionSpec as P

learn_rate = 0.5
LANE = 128
PLAN = (2, 18, 3, 1)
SUB = 8
NB = 2
PIECES = 4
LATE = 2
MESH = pl.DeviceIdType.MESH
NN = (((1,), (0,)), ((), ()))
NT = (((1,), (1,)), ((), ()))


def exact_dot(left, right, dims):
    return lax.dot_general(
        left, right, dims, precision=lax.Precision.HIGHEST, preferred_element_type=jnp.float32
    )


def fast_dot(left, right, dims):
    return lax.dot_general(left, right, dims, preferred_element_type=jnp.float32)


def halves(value):
    high = value.astype(jnp.bfloat16)
    low = (value - high.astype(jnp.float32)).astype(jnp.bfloat16)
    return high, low


def gather_kernel(
    reps, feats, rank, rows, cols, total_feat,
    basis_hbm, stream_hbm, gram_ref, mh_ref, ml_ref,
    m_ref, w_ref, x_ref, whl_ref, sums_refs, recv_refs, av_ref,
    pay_ref, half_recv, half_sum, z_recv, full_ref,
    g_ref, g_recv,
    load_f, load_w, load_x_sem, ring_send, ring_recv, more_recv, core_send, core_recv, z_send, z_recv_sem,
    g_send, g_recv_sem, hello_sem,
):
    bits = reps.bit_length() - 1
    chunk = LANE * reps
    chunks = cols // chunk
    zs = feats // 2
    me = lax.axis_index("rep")
    feat = lax.axis_index("feat")
    core = feat % 2
    zpos = feat // 2
    eta = learn_rate / rows
    scale = jnp.sqrt(jnp.float32(total_feat))

    def rep_peer(b):
        bit = (me // (1 << b)) % 2
        return me + (1 - 2 * bit) * (1 << b), bit

    rep_ids = [(rep_peer(b)[0], feat) for b in range(bits)]
    core_id = (me, feat + 1 - 2 * core)
    z_ids = [(me, ((zpos + d) % zs) * 2 + core) for d in range(1, zs)]

    beside = (zpos > 0).astype(jnp.int32) + (zpos < zs - 1).astype(jnp.int32)

    def tell_beside(sem):
        for ahead, there in ((-1, zpos > 0), (1, zpos < zs - 1)):

            @pl.when(there)
            def _():
                pl.semaphore_signal(
                    sem, inc=1, device_id=(me, feat + 2 * ahead), device_id_type=MESH
                )

    barrier = pltpu.get_barrier_semaphore()
    for peer in rep_ids + [core_id]:
        pl.semaphore_signal(barrier, inc=1, device_id=peer, device_id_type=MESH)
    tell_beside(barrier)
    front = chunk * (chunks // 2)
    load_front = pltpu.make_async_copy(basis_hbm.at[:, 0:front], w_ref.at[:, 0:front], load_f)
    load_front.start()
    load_basis = pltpu.make_async_copy(basis_hbm.at[:, front:cols], w_ref.at[:, front:cols], load_w)
    load_basis.start()
    load_x = pltpu.make_async_copy(stream_hbm, x_ref, load_x_sem)
    load_x.start()
    pl.semaphore_wait(barrier, bits + 1 + beside)

    def link(src, dst, send_sem, recv_sem, peer):
        return pltpu.make_async_remote_copy(
            src_ref=src, dst_ref=dst, send_sem=send_sem, recv_sem=recv_sem,
            device_id=peer, device_id_type=MESH,
        )

    def remote(*args):
        copy = link(*args)
        copy.start()
        return copy

    def at(off, width):
        return pl.ds(pl.multiple_of(off, LANE), width)

    def order(c):
        return [(c + i) % bits for i in range(bits)]

    keeps = []
    for c in range(chunks):
        off = c * chunk
        rec = []
        for i, b in enumerate(order(c)):
            width = chunk >> (i + 1)
            bit = rep_peer(b)[1]
            off = off + bit * width
            rec.append(off)
        keeps.append(rec)

    ring = {}

    def send_scatter(c, i):
        b = order(c)[i]
        width = chunk >> (i + 1)
        bit = rep_peer(b)[1]
        other = (1 - bit) * width
        if i == 0:
            src = w_ref.at[:, at(c * chunk + other, width)]
        else:
            src = sums_refs[i - 1].at[:, at(c * 2 * width + other, width)]
        dst = recv_refs[i].at[:, c * width:(c + 1) * width]
        ring[c, i] = remote(src, dst, ring_send.at[0], ring_recv.at[i, c], rep_ids[b])

    def take_scatter(c, i):
        b = order(c)[i]
        width = chunk >> (i + 1)
        bit = rep_peer(b)[1]
        ring[c, i].wait_recv()
        if i == 0:
            own = w_ref[:, at(c * chunk + bit * width, width)]
        else:
            own = sums_refs[i - 1][:, at(c * 2 * width + bit * width, width)]
        total = own + recv_refs[i][:, c * width:(c + 1) * width]
        if i == bits - 1:
            av_ref[:, at(keeps[c][i], width)] = total / reps
        else:
            sums_refs[i][:, c * width:(c + 1) * width] = total

    def send_gather(c, i):
        s = bits - 1 - i
        b = order(c)[s]
        width = chunk >> (s + 1)
        piece = av_ref.at[:, at(keeps[c][s], width)]
        k = bits + i
        if i == 0:
            done = ring_recv.at[0, c]
        elif bits == 2 and c > 0:
            done = ring_recv.at[1, c - 1]
        else:
            done = more_recv.at[i - 1, c]
        ring[c, k] = remote(piece, piece, ring_send.at[1], done, rep_ids[b])

    load_front.wait()
    for c in range(chunks):
        if c == chunks // 2:
            load_basis.wait()
        send_scatter(c, 0)
    rounds = zs - 2
    if rounds > 0:
        tell_beside(hello_sem.at[0])

    def step(c, i):
        if i < bits:
            take_scatter(c, i)
        else:
            ring[c, i].wait_recv()
        if i + 1 < bits:
            send_scatter(c, i + 1)
        elif i + 1 < 2 * bits:
            send_gather(c, i + 1 - bits)

    pending = [(c, i) for i in range(2 * bits - 1) for c in range(chunks)]
    place = [0]

    def advance(count):
        for _ in range(count):
            if place[0] < len(pending):
                step(*pending[place[0]])
                place[0] += 1

    high, low = halves(w_ref[...])
    whl_ref[0:rank, :] = high
    whl_ref[rank:2 * rank, :] = low
    load_x.wait()
    x_all = x_ref[...]
    wx = fast_dot(whl_ref[...], x_all, NT)
    wx = wx[0:rank] + wx[rank:2 * rank]
    pay_ref[0:rank, :] = wx[:, 0:rows]
    pay_ref[rank:2 * rank, :] = wx[:, rows:2 * rows]
    pay_ref[2 * rank:2 * rank + rows, :] = fast_dot(x_ref[0:rows, :], x_ref[rows:2 * rows, :], NT)

    half = rank + rows // 2
    give = pl.ds(pl.multiple_of((1 - core) * half, 8), half)
    keep = pl.ds(pl.multiple_of(core * half, 8), half)
    core_copy = remote(pay_ref.at[give, :], half_recv, core_send, core_recv.at[0], core_id)
    advance(PLAN[0])
    core_copy.wait_recv()
    half_sum[...] = pay_ref[keep, :] + half_recv[...]
    for k in range(rounds):
        pl.semaphore_wait(hello_sem.at[k], beside)
        if k + 1 < rounds:
            tell_beside(hello_sem.at[k + 1])
    for d in range(zs - 1):
        remote(half_sum, z_recv.at[d], z_send, z_recv_sem, z_ids[d])
    advance(PLAN[1])
    total = half_sum[...]
    z_all = link(z_recv, z_recv, z_send, z_recv_sem, core_id)
    z_all.wait_recv()
    for d in range(zs - 1):
        total = total + z_recv[d]
    full_ref[keep, :] = total
    share = remote(full_ref.at[keep, :], full_ref.at[keep, :], core_send, core_recv.at[1], core_id)
    advance(PLAN[2])
    share.wait_recv()

    first = full_ref[0:rank, :]
    second = full_ref[rank:2 * rank, :]
    cross = full_ref[2 * rank:2 * rank + rows, :]
    proj0 = first / scale
    cov0 = exact_dot(proj0, proj0, NT)
    drive1 = exact_dot(proj0, cross, NN)
    proj1 = (second + eta * (drive1 - exact_dot(cov0, second, NN))) / scale
    cov1 = exact_dot(proj1, proj1, NT)
    advance(PLAN[3])
    k_w = eta * (eta * exact_dot(cov1, cov0, NN) - cov0 - cov1)
    k_x0 = eta * (proj0 - eta * exact_dot(cov1, proj0, NN))
    k_x1 = eta * proj1
    kwh, kwl = halves(k_w)
    kx = jnp.concatenate([k_x0, k_x1], axis=1)
    kxh, kxl = halves(kx)
    kx2 = jnp.concatenate([kxh, kxl], axis=0)
    kw2 = jnp.concatenate([kwh, kwl], axis=0)

    def unmixed(c):
        cut = slice(c * chunk, (c + 1) * chunk)
        part = fast_dot(kx2, x_ref[:, cut], NN) + fast_dot(kw2, whl_ref[0:rank, cut], NN)
        part = part[0:rank] + part[rank:2 * rank] + fast_dot(kwh, whl_ref[rank:2 * rank, cut], NN)
        m_ref[:, cut] = part

    for c in range(chunks):
        unmixed(c)
        advance(1)
    advance(len(pending))

    slim = [jnp.zeros((2 * rank, rank), jnp.float32)]
    full = [jnp.zeros((rank, 2 * rank), jnp.float32)]

    def mix(off, width, late):
        cut = at(off, width)
        mh, ml = halves(m_ref[:, cut] + av_ref[:, cut])
        mh_ref[:, cut] = mh
        ml_ref[:, cut] = ml
        both = jnp.concatenate([mh, ml], axis=0)
        if late:
            part = fast_dot(both, jnp.concatenate([mh, mh], axis=0), NT)
            part = part[0:rank] + part[rank:2 * rank]
            full[0] = full[0] + (part + fast_dot(mh, jnp.concatenate([ml, ml], axis=0), NT))
        else:
            slim[0] = slim[0] + fast_dot(both, mh, NT)

    wide = chunk // 2
    for c in range(chunks):
        mix(keeps[c][0], wide, False)
    for c in range(chunks):
        if c == chunks - LATE:
            low_part = slim[0][rank:2 * rank]
            early = slim[0][0:rank] + (low_part + low_part.T)
            full[0] = full[0] + jnp.concatenate([early, early], axis=1)
        ring[c, 2 * bits - 1].wait_recv()
        mix(2 * c * chunk + wide - keeps[c][0], wide, c >= chunks - LATE)
    hr = rank // 2
    gram = full[0] * (1.0 / total_feat)
    lane = lax.broadcasted_iota(jnp.int32, (hr, 2 * rank), 1)
    g_ref[...] = jnp.where(lane < rank, gram[0:hr], gram[hr:rank])
    upper = (2 * zpos) // zs
    for j in range(zs - 1):
        far = upper * (j + (j >= zpos).astype(jnp.int32))
        near = (1 - upper) * (zs - 1 - j - (zs - 1 - j <= zpos).astype(jnp.int32))
        peer = far + near
        slot = (peer - zpos + zs) % zs - 1
        for k in range(2):
            remote(
                g_ref, g_recv.at[2 * slot + k], g_send, g_recv_sem,
                (me, peer * 2 + (core + k) % 2),
            )
    remote(g_ref, g_recv.at[2 * zs - 2], g_send, g_recv_sem, core_id)
    sent = cols - cols // reps
    g_all = link(g_recv, g_recv, g_send, g_recv_sem, core_id)
    link(w_ref.at[:, 0:sent], w_ref.at[:, 0:sent], ring_send.at[0], core_recv.at[0], core_id).wait_send()
    link(w_ref.at[:, 0:sent], w_ref.at[:, 0:sent], ring_send.at[1], core_recv.at[0], core_id).wait_send()
    link(pay_ref, pay_ref, core_send, core_recv.at[0], core_id).wait_send()
    z_all.wait_send()
    g_all.wait_send()
    g_all.wait_recv()
    total = g_ref[...]
    for d in range(2 * zs - 1):
        total = total + g_recv[d]
    gram_ref[...] = total


def lanes(block, lane):
    return jnp.broadcast_to(block[:, lane:lane + 1], block.shape)

def row(block, r):
    return jnp.broadcast_to(block[r:r + 1, :], block.shape)

def panel(blocks, first, nb, col, ids):
    w = SUB * nb
    last = len(blocks)
    own = [blocks[first + v] for v in range(nb)]
    keep = ids < w
    d = [[jnp.where(keep, lanes(own[v], col + k), 0.0) for v in range(nb)] for k in range(w)]
    c = {i: [lanes(blocks[i], col + k) for k in range(w)] for i in range(first + nb, last)}
    done = []
    for p in range(0, w, 2):
        v, s = divmod(p, SUB)
        a00, a10, a11 = row(d[p][v], s), row(d[p][v], s + 1), row(d[p + 1][v], s + 1)
        idet = 1.0 / (a00 * a11 - a10 * a10)
        i00, i01, i11 = a11 * idet, -(a10 * idet), a00 * idet
        at0, pair = ids == s, (ids == s) | (ids == s + 1)
        e0 = [d[p][u] * i00 + d[p + 1][u] * i01 for u in range(nb)]
        e1 = [d[p][u] * i01 + d[p + 1][u] * i11 for u in range(nb)]
        e0[v] = jnp.where(pair, jnp.where(at0, -i00, -i01), e0[v])
        e1[v] = jnp.where(pair, jnp.where(at0, -i01, -i11), e1[v])

        def step(x):
            t0, t1 = row(x[v], s), row(x[v], s + 1)
            base = [jnp.where(pair, 0.0, x[u]) if u == v else x[u] for u in range(nb)]
            return t0, t1, [base[u] - (e0[u] * t0 + e1[u] * t1) for u in range(nb)]

        r0, r1, own = step(own)
        ratio = a10 / a00
        done.append(r0 * lax.rsqrt(a00))
        done.append((r1 - ratio * r0) * lax.rsqrt(a11 - ratio * a10))
        for k in range(p + 2, w):
            d[k] = step(d[k])[2]
    if c:
        z = [row(own[p // SUB], p % SUB) for p in range(w)]
        for i in c:
            parts = [c[i][p] * z[p] for p in range(w)]
            while len(parts) > 1:
                parts = [parts[q] + parts[q + 1] for q in range(0, len(parts), 2)]
            blocks[i] = blocks[i] - parts[0]
    res = []
    for v in range(nb):
        out = done[v * SUB]
        for s in range(1, SUB):
            out = jnp.where(ids == s, done[v * SUB + s], out)
        res.append(out)
    return res
def solve_kernel(rank, cols, gram_ref, mh_ref, ml_ref, out_hbm, ph_ref, pl_ref, o_ref, out_sem):
    hr = rank // 2
    n = rank // SUB
    half = n // 2
    lane = lax.broadcasted_iota(jnp.int32, (SUB, 2 * rank), 1)
    ids = lax.broadcasted_iota(jnp.int32, (SUB, 2 * rank), 0)
    both = gram_ref[...]
    zero = jnp.zeros((SUB, rank), jnp.float32)
    top = [both[i * SUB:(i + 1) * SUB, :] for i in range(half)]
    low = [jnp.concatenate([t[:, rank:2 * rank], zero], axis=1) for t in top]
    blocks = [
        jnp.where(lane < rank, top[i], jnp.where(lane == rank + ids + i * SUB, 1.0, 0.0))
        for i in range(half)
    ] + low
    width = cols // PIECES

    def send(lo, p):
        cut = slice(p * width, (p + 1) * width)
        copy = pltpu.make_async_copy(
            o_ref.at[lo:lo + hr, cut], out_hbm.at[lo:lo + hr, cut], out_sem
        )
        copy.start()

    def eliminate(first):
        scaled = []
        for b in range(first, first + half, NB):
            scaled += panel(blocks, b, NB, b * SUB, ids)
        return scaled

    scaled = eliminate(0)
    left = jnp.concatenate(scaled + blocks[half:], axis=0)[:, rank:rank + hr]
    th, tl = halves(left)
    thl = jnp.concatenate([th, tl], axis=0)
    for p in range(PIECES):
        cut = slice(p * width, (p + 1) * width)
        part = fast_dot(thl, mh_ref[0:hr, cut], NN)
        part = part[0:rank] + part[rank:2 * rank] + fast_dot(th, ml_ref[0:hr, cut], NN)
        o_ref[0:hr, cut] = part[0:hr]
        send(0, p)
        rest = part[hr:rank] + mh_ref[hr:rank, cut].astype(jnp.float32)
        rest = rest + ml_ref[hr:rank, cut].astype(jnp.float32)
        ph_ref[:, cut], pl_ref[:, cut] = halves(rest)
    for i in range(half):
        unit = jnp.where(lane % hr == ids + i * SUB, 1.0, 0.0)
        pivots = (lane >= hr) & (lane < rank)
        blocks[half + i] = jnp.where(pivots, blocks[half + i], unit)
    left = jnp.concatenate(eliminate(half), axis=0)
    wide_lane = lax.broadcasted_iota(jnp.int32, (hr, 2 * rank), 1)
    left = jnp.where((wide_lane >= hr) & (wide_lane < rank), 0.0, left)
    th, tl = halves(left)
    low_lane = (wide_lane >= rank) & (wide_lane < rank + hr)
    mixed = jnp.where(low_lane, tl.astype(jnp.float32), th.astype(jnp.float32))
    mixed = mixed.astype(jnp.bfloat16)
    for p in range(PIECES):
        cut = slice(p * width, (p + 1) * width)
        ph, pl_ = ph_ref[:, cut], pl_ref[:, cut]
        o_ref[hr:rank, cut] = fast_dot(mixed, jnp.concatenate([ph, pl_, ph, pl_], axis=0), NN)
        send(hr, p)
    pltpu.make_async_copy(o_ref, out_hbm, out_sem).wait()


def per_device(basis, stream):
    reps = lax.axis_size("rep")
    feats = lax.axis_size("feat")
    start = basis[0]
    steps, rows, cols = stream.shape[1:]
    batches = stream[0].reshape(steps * rows, cols)
    rank = start.shape[0]
    bits = reps.bit_length() - 1
    chunk = LANE * reps
    chunks = cols // chunk
    zs = feats // 2
    half = rank + rows // 2
    f32 = jnp.float32
    vm = pltpu.VMEM
    hr = rank // 2
    dma = pltpu.SemaphoreType.DMA
    gram, mh, ml = pl.pallas_call(
        functools.partial(gather_kernel, reps, feats, rank, rows, cols, cols * feats),
        out_shape=(
            pltpu.VMEM((hr, 2 * rank), f32),
            pltpu.VMEM((rank, cols), jnp.bfloat16),
            pltpu.VMEM((rank, cols), jnp.bfloat16),
        ),
        in_specs=[pl.BlockSpec(memory_space=pl.ANY)] * 2,
        out_specs=(pl.BlockSpec(memory_space=pltpu.VMEM),) * 3,
        scratch_shapes=[
            vm((rank, cols), f32),
            vm((rank, cols), f32),
            vm((steps * rows, cols), jnp.bfloat16),
            vm((2 * rank, cols), jnp.bfloat16),
            [vm((rank, cols >> (i + 1)), f32) for i in range(bits)],
            [vm((rank, cols >> (i + 1)), f32) for i in range(bits)],
            vm((rank, cols), f32),
            vm((2 * half, rows), f32),
            vm((half, rows), f32),
            vm((half, rows), f32),
            vm((zs - 1, half, rows), f32),
            vm((2 * half, rows), f32),
            vm((hr, 2 * rank), f32),
            vm((2 * zs - 1, hr, 2 * rank), f32),
            dma,
            dma,
            dma,
            dma((2,)),
            dma((bits, chunks)),
            dma((1, 1)) if bits == 2 else dma((bits - 1, chunks)),
            dma,
            dma((2,)),
            dma,
            dma,
            dma,
            dma,
            pltpu.SemaphoreType.REGULAR((max(zs - 2, 1),)),
        ],
        compiler_params=pltpu.CompilerParams(
            collective_id=0, has_side_effects=True,
        ),
    )(start, batches)
    result = pl.pallas_call(
        functools.partial(solve_kernel, rank, cols),
        out_shape=jax.ShapeDtypeStruct((rank, cols), f32),
        in_specs=[pl.BlockSpec(memory_space=pltpu.VMEM)] * 3,
        out_specs=pl.BlockSpec(memory_space=pl.ANY),
        scratch_shapes=[
            vm((hr, cols), jnp.bfloat16),
            vm((hr, cols), jnp.bfloat16),
            vm((rank, cols), f32),
            dma,
        ],
    )(
        pltpu.with_memory_space_constraint(gram, pltpu.VMEM),
        pltpu.with_memory_space_constraint(mh, pltpu.VMEM),
        pltpu.with_memory_space_constraint(ml, pltpu.VMEM),
    )
    return result[None]


def solution(mesh):
    placed = (P("rep", None, "feat"), P("rep", None, None, "feat"))
    return jax.shard_map(
        per_device, mesh=mesh, in_specs=placed, out_specs=P("rep", None, "feat"), check_vma=False
    )
```
